32 devices in a mesh: rows: 8 (over y, x, core), cols: 4 (over z).
Axes of the slice: x: 2, y: 2, z: 4, core: 2. Of those that a mesh axis runs over, the one named last changes fastest.
Arguments:
- surface_field: float32 [4096, 8192], P('rows', 'cols'), may hold values from -20 to 30
- land_words: int32 [4096, 256], P('rows', 'cols'), may hold values from -2147483648 to 2147483646
Outputs:
- level_one: float32 [2048, 4096], P('rows', 'cols')
- level_two: float32 [1024, 2048], P('rows', 'cols')
- level_three: float32 [512, 1024], P('rows', 'cols')
- level_four: float32 [256, 512], P('rows', 'cols')
- level_means: float32 [4], replicated
- level_maxima: float32 [4], replicated
The draws below stay inside these ranges and needn't reach their ends.
All inputs are finite; a program needn't handle non-finite values.
Results may differ from the reference program's by a relative error of at most 0.0001.
Values sent between devices are 32-bit elements; how exact they have to be, the bound alone decides.
A program may use at most 128 MiB of HBM per device.

```python
import math
import jax
import jax.numpy as jnp

NY = 4096
NX = 8192


def draw_surface_field(key, part):
    noise_key = jax.random.fold_in(jax.random.fold_in(key, 11), 0)
    rows_frac = jnp.arange(NY, dtype=jnp.float32) / NY
    cols_frac = jnp.arange(NX, dtype=jnp.float32) / NX
    trend = (1.0 + 2.0 * rows_frac)[:, None] * (1.0 + 2.0 * cols_frac)[None, :]
    noise = jnp.clip(jax.random.normal(noise_key, (NY, NX), jnp.float32), -6.0, 6.0)
    return (trend + noise).astype(jnp.float32)


def touch_ends(values, key, smallest, top_value):
    index_at = [jax.random.randint(jax.random.fold_in(key, axis), (), 0, length) for axis, length in enumerate(values.shape)]
    main_axis = values.shape.index(max(values.shape))
    next_to = index_at[:main_axis] + [(index_at[main_axis] + 1) % values.shape[main_axis]] + index_at[main_axis + 1:]
    return values.at[tuple(index_at)].set(smallest).at[tuple(next_to)].set(top_value)


def setup_inputs(seed: int = 0) -> dict:
    splits = jax.random.split(jax.random.key(seed), 3)
    surface_field = draw_surface_field(jax.random.fold_in(splits[2], 71), 0)
    land_words = touch_ends(jax.random.randint(splits[1], (NY, NX // 32), -2147483648, 2147483647), jax.random.fold_in(splits[1], 1), -2147483648, 2147483646).astype(jnp.int32)
    return dict(surface_field=surface_field, land_words=land_words)


stencil_weights = (0.125, 0.375, 0.375, 0.125)
floor_value = 0.05
mean_eps = 1e-6


def coarsen(extended):
    count_rows = (extended.shape[1] - 2) // 2
    count_cols = (extended.shape[2] - 2) // 2
    across = stencil_weights[0] * extended[:, :, 0:2 * count_cols:2]
    for offset in range(1, 4):
        across = across + stencil_weights[offset] * extended[:, :, offset:offset + 2 * count_cols:2]
    downward = stencil_weights[0] * across[:, 0:2 * count_rows:2, :]
    for offset in range(1, 4):
        downward = downward + stencil_weights[offset] * across[:, offset:offset + 2 * count_rows:2, :]
    return downward


def finish(partial_value):
    values = partial_value[0] / jnp.maximum(partial_value[1], floor_value)
    covers = partial_value[1]
    return values, covers, jnp.stack([covers * values, covers])


def reference(surface_field, land_words):
    expanded = jnp.repeat(land_words, 32, axis=1)
    shifts = jnp.arange(expanded.shape[1], dtype=jnp.int32) % 32
    land_flag = jnp.bitwise_and(jnp.right_shift(expanded, shifts[None, :]), 1)
    rows_index = jnp.arange(NY, dtype=jnp.int32).astype(jnp.float32)
    latitude = ((rows_index + 0.5) / NY - 0.5) * math.pi
    covers = land_flag.astype(jnp.float32) * jnp.cos(latitude)[:, None]
    stacked = jnp.stack([covers * surface_field, covers])
    outputs = []
    weighted = []
    totals = []
    maxima = []
    for level_step in range(4):
        wrapped = jnp.concatenate([stacked[:, :, -1:], stacked, stacked[:, :, :1]], axis=2)
        padded = jnp.pad(wrapped, ((0, 0), (1, 1), (0, 0)))
        values, covers, stacked = finish(coarsen(padded))
        outputs.append(values)
        weighted.append(jnp.sum(stacked[0]))
        totals.append(jnp.sum(covers))
        maxima.append(jnp.max(values))
    level_means = jnp.stack(weighted) / (jnp.stack(totals) + mean_eps)
    return outputs[0], outputs[1], outputs[2], outputs[3], level_means, jnp.stack(maxima)
```

```python
import functools
import math

import jax
import jax.numpy as jnp
from jax import lax
from jax.experimental import pallas as pl
from jax.experimental.pallas import tpu as pltpu
from jax.sharding import PartitionSpec as P

stencil_weights = (0.125, 0.375, 0.375, 0.125)
floor_value = 0.05
mean_eps = 1e-06
LEVELS = 4
LANES = 128
HALO = 16
MESH = pl.DeviceIdType.MESH


def kernel(
    row_devices,
    col_devices,
    field,
    land_words,
    level_one,
    level_two,
    level_three,
    level_four,
    means_ref,
    maxima_ref,
    land,
    fine,
    words,
    cosines,
    send_left,
    send_right,
    from_left,
    from_right,
    rows_top,
    rows_bottom,
    land_top,
    land_bottom,
    p0,
    c0,
    p1,
    c1,
    p2,
    c2,
    p3,
    c3,
    split,
    stat_own,
    stat_all,
    load_sem,
    land_sem,
    halo_send,
    halo_recv,
    stat_send,
    stat_recv,
):
    rows, cols = field.shape
    tiles = cols // LANES
    count_words = land_words.shape[0]
    row_at = lax.axis_index("rows")
    col_at = lax.axis_index("cols")
    total_rows = rows * row_devices

    def device(down, right):
        return (
            lax.rem(row_at + down + row_devices, row_devices),
            lax.rem(col_at + right + col_devices, col_devices),
        )

    others = [
        (down, right)
        for down in range(row_devices)
        for right in range(col_devices)
        if (down, right) != (0, 0)
    ]

    def load(tile):
        start = tile * LANES
        if not isinstance(tile, int):
            start = pl.multiple_of(start, LANES)
        return pltpu.make_async_copy(
            field.at[:, pl.ds(start, LANES)], fine.at[tile], load_sem.at[tile]
        )

    barrier = pltpu.get_barrier_semaphore()
    for down, right in others:
        pl.semaphore_signal(barrier, inc=1, device_id=device(down, right), device_id_type=MESH)

    land_load = pltpu.make_async_copy(land_words, land, land_sem)
    land_load.start()
    load(0).start()
    load(tiles - 1).start()
    for tile in range(1, tiles - 1):
        load(tile).start()

    def upright(array):
        if count_words < LANES:
            filler = jnp.zeros((LANES - count_words, array.shape[1]), jnp.int32)
            array = jnp.concatenate([array, filler], axis=0)
        return jnp.transpose(array)

    land_load.wait()
    words[HALO : HALO + rows, :] = upright(land[...])
    lane = lax.broadcasted_iota(jnp.int32, (8, LANES), 1)

    def flags(tile, start, count):
        lanes = lax.broadcasted_iota(jnp.int32, (count, LANES), 1)
        place = tile * (LANES // 32) + lax.shift_right_logical(lanes, 5)
        word = jnp.take_along_axis(
            words[pl.ds(start, count), :], place, axis=1, mode="promise_in_bounds"
        )
        return jnp.bitwise_and(
            lax.shift_right_logical(word, jnp.bitwise_and(lanes, 31)), 1
        ).astype(jnp.float32)

    blocks = -(-(rows + 2 * HALO) // LANES)
    packed = (8 * (-(-blocks // 8)), LANES)
    row_index = (
        row_at * rows
        - HALO
        + lax.broadcasted_iota(jnp.int32, packed, 0) * LANES
        + lax.broadcasted_iota(jnp.int32, packed, 1)
    )
    latitude = ((row_index.astype(jnp.float32) + 0.5) / total_rows - 0.5) * math.pi
    on_globe = jnp.logical_and(row_index >= 0, row_index < total_rows)
    packed_cosines = jnp.where(on_globe, jnp.cos(latitude), 0.0)
    for block in range(blocks):
        size = min(LANES, rows + 2 * HALO - block * LANES)
        spread = jnp.broadcast_to(packed_cosines[block : block + 1, :], (LANES, LANES))
        cosines[block * LANES : block * LANES + size, :] = jnp.transpose(spread)[0:size, :]

    load(0).wait()
    send_left[0:HALO, :] = jnp.transpose(fine[0])[0:HALO, :]
    send_left[HALO:, :] = jnp.transpose(flags(0, HALO, rows))[0:HALO, :]
    load(tiles - 1).wait()
    send_right[0:HALO, :] = jnp.transpose(fine[tiles - 1])[LANES - HALO :, :]
    send_right[HALO:, :] = jnp.transpose(flags(tiles - 1, HALO, rows))[LANES - HALO :, :]

    zero_pad = ((p0, c0, 8), (p1, c1, 16), (p2, c2, 16), (p3, c3, 16))
    for product, cover, width in zero_pad:
        for ref in (product, cover):
            shape = (ref.shape[0], width, LANES)
            ref[:, 0:width, :] = jnp.zeros(shape, jnp.float32)
            ref[:, ref.shape[1] - width :, :] = jnp.zeros(shape, jnp.float32)

    pl.semaphore_wait(barrier, len(others))
    plan = (
        (field.at[rows - HALO : rows, :], rows_top, (1, 0)),
        (field.at[0:HALO, :], rows_bottom, (-1, 0)),
        (land.at[:, rows - LANES : rows], land_top, (1, 0)),
        (land.at[:, 0:LANES], land_bottom, (-1, 0)),
        (send_left, from_right.at[:, LANES : LANES + rows], (0, -1)),
        (send_right, from_left.at[:, LANES : LANES + rows], (0, 1)),
        (send_left.at[:, 0:LANES], from_right.at[:, LANES + rows :], (-1, -1)),
        (send_right.at[:, 0:LANES], from_left.at[:, LANES + rows :], (-1, 1)),
        (send_left.at[:, rows - LANES :], from_right.at[:, 0:LANES], (1, -1)),
        (send_right.at[:, rows - LANES :], from_left.at[:, 0:LANES], (1, 1)),
    )
    copies = []
    for place, (source, target, (down, right)) in enumerate(plan):
        copy = pltpu.make_async_remote_copy(
            src_ref=source,
            dst_ref=target,
            send_sem=halo_send.at[place],
            recv_sem=halo_recv.at[place],
            device_id=device(down, right),
            device_id_type=MESH,
        )
        copy.start()
        copies.append(copy)

    def own_tile(tile):
        for start in range(0, rows, 64):
            cover = flags(tile, HALO + start, 64) * cosines[HALO + start : HALO + start + 64, :]
            c0[tile + 1, 24 + start : 88 + start, :] = cover
            p0[tile + 1, 24 + start : 88 + start, :] = cover * fine[tile, start : start + 64, :]

    own_tile(0)
    own_tile(tiles - 1)

    @pl.loop(1, tiles - 1)
    def _(tile):
        load(tile).wait()
        own_tile(tile)

    for copy in copies:
        copy.wait()

    words[0:HALO, :] = upright(land_top[...])[LANES - HALO :, :]
    words[HALO + rows :, :] = upright(land_bottom[...])[0:HALO, :]
    for landed, at in ((rows_top, 0), (rows_bottom, HALO + rows)):
        for tile in range(tiles):
            cover = flags(tile, at, HALO) * cosines[at : at + HALO, :]
            c0[tile + 1, 8 + at : 8 + at + HALO, :] = cover
            p0[tile + 1, 8 + at : 8 + at + HALO, :] = (
                cover * landed[:, tile * LANES : (tile + 1) * LANES]
            )
    filler = jnp.zeros((LANES - HALO, rows + 2 * LANES), jnp.float32)
    first = LANES - HALO
    last = LANES + rows + HALO
    for packet, tile, at_end in ((from_left, 0, True), (from_right, tiles + 1, False)):
        sides = []
        for part in (packet[0:HALO, :], packet[HALO:, :]):
            pieces = [filler, part] if at_end else [part, filler]
            sides.append(jnp.transpose(jnp.concatenate(pieces, axis=0))[first:last, :])
        cover = sides[1] * cosines[...]
        c0[tile, 8 : 8 + rows + 2 * HALO, :] = cover
        p0[tile, 8 : 8 + rows + 2 * HALO, :] = cover * sides[0]

    band_row = lax.broadcasted_iota(jnp.int32, (4 * LANES, LANES), 0)
    band_col = lax.broadcasted_iota(jnp.int32, (4 * LANES, LANES), 1)
    tap = band_row - (LANES - 1) - 2 * band_col
    band = jnp.where(
        jnp.logical_or(tap == 0, tap == 3),
        stencil_weights[0],
        jnp.where(jnp.logical_or(tap == 1, tap == 2), stencil_weights[1], 0.0),
    ).astype(jnp.bfloat16)

    stats = []
    sources = ((p0, c0), (p1, c1), (p2, c2), (p3, c3))
    outputs = (level_one, level_two, level_three, level_four)
    for level in range(LEVELS):
        product_in, cover_in = sources[level]
        output = outputs[level]
        own = output.shape[0]
        count = own + 16
        tiles_in = product_in.shape[0]
        tiles_out = output.shape[1] // LANES

        @pl.loop(0, tiles_in)
        def _(tile):
            offset = pl.multiple_of(tile * LANES, LANES)
            for place, ref in enumerate((product_in, cover_in)):
                taps = [ref[tile, pl.ds(7 + a, count, stride=2), :] for a in range(4)]
                down = stencil_weights[0] * (taps[0] + taps[3]) + stencil_weights[1] * (
                    taps[1] + taps[2]
                )
                high = down.astype(jnp.bfloat16)
                low = (down - high.astype(jnp.float32)).astype(jnp.bfloat16)
                at = 2 * place * count
                split[at : at + count, pl.ds(offset, LANES)] = high
                split[at + count : at + 2 * count, pl.ds(offset, LANES)] = low

        index = row_at * own - 8 + lax.broadcasted_iota(jnp.int32, (count, LANES), 0)
        inside = jnp.logical_and(index >= 0, index < own * row_devices)

        def across(start, width, table):
            result = jnp.dot(
                split[0 : 4 * count, pl.ds(start, width)],
                table,
                preferred_element_type=jnp.float32,
            )
            num = result[0:count] + result[count : 2 * count]
            den = result[2 * count : 3 * count] + result[3 * count :]
            value = num / jnp.maximum(den, floor_value)
            cover = jnp.where(inside, den, 0.0)
            return value, cover, cover * value

        def keep(tile, cover, product):
            if level + 1 < LEVELS:
                product_out, cover_out = sources[level + 1]
                product_out[tile, 16 : 16 + count, :] = product
                cover_out[tile, 16 : 16 + count, :] = cover

        if level + 1 < LEVELS:
            value, cover, product = across(0, 2 * LANES, band[2 * LANES :])
            keep(0, cover, product)
            value, cover, product = across((tiles_in - 2) * LANES, 2 * LANES, band[: 2 * LANES])
            keep(tiles_out + 1, cover, product)

        def own_columns(tile, carry):
            weighted, total, largest = carry
            value, cover, product = across(
                pl.multiple_of(tile * 2 * LANES, 2 * LANES), 4 * LANES, band
            )
            keep(tile + 1, cover, product)
            output[:, pl.ds(pl.multiple_of(tile * LANES, LANES), LANES)] = value[8 : 8 + own]

            def parts(array):
                return array[8 : 8 + own].reshape(own // 8, 8, LANES)

            return (
                weighted + jnp.sum(parts(product), axis=0),
                total + jnp.sum(parts(cover), axis=0),
                jnp.maximum(largest, jnp.max(parts(value), axis=0)),
            )

        zero = jnp.zeros((8, LANES), jnp.float32)
        start = (zero, zero, jnp.full((8, LANES), -jnp.inf, jnp.float32))
        stats.append(lax.fori_loop(0, tiles_out, own_columns, start))

    row = lax.broadcasted_iota(jnp.int32, (8, LANES), 0)
    own = jnp.zeros((8, LANES), jnp.float32)
    for kind, reduce in ((0, jnp.sum), (1, jnp.sum), (2, jnp.max)):
        tile = jnp.zeros((8, LANES), jnp.float32)
        for level in range(LEVELS):
            tile = jnp.where(row == level, reduce(stats[level][kind], axis=0, keepdims=True), tile)
        own = jnp.where(lane == row + kind * LEVELS, reduce(tile, axis=1, keepdims=True), own)
    own = jnp.where(row < LEVELS, own, 0.0)
    stat_own[...] = jnp.broadcast_to(jnp.sum(own, axis=0, keepdims=True), (8, LANES))
    copies = []
    for place, (down, right) in enumerate(others):
        copy = pltpu.make_async_remote_copy(
            src_ref=stat_own.at[0:1],
            dst_ref=stat_all.at[place : place + 1],
            send_sem=stat_send.at[place],
            recv_sem=stat_recv.at[place],
            device_id=device(down, right),
            device_id_type=MESH,
        )
        copy.start()
        copies.append(copy)
    for copy in copies:
        copy.wait()
    first = stat_own[0:1, :]
    summed = first + jnp.sum(stat_all[...], axis=0, keepdims=True)
    largest = jnp.maximum(first, jnp.max(stat_all[...], axis=0, keepdims=True))
    summed = jnp.broadcast_to(summed, (8, LANES))
    largest = jnp.broadcast_to(largest, (8, LANES))

    def pick(array, kind):
        here = jnp.logical_and(lane == row + kind * LEVELS, row < LEVELS)
        return jnp.sum(jnp.where(here, array, 0.0), axis=1, keepdims=True)

    level_means = pick(summed, 0) / (pick(summed, 1) + mean_eps)
    diagonal = jnp.logical_and(lane == row, row < LEVELS)
    means_ref[...] = jnp.sum(jnp.where(diagonal, level_means, 0.0), axis=0)[0:LEVELS]
    maxima_ref[...] = jnp.sum(jnp.where(diagonal, pick(largest, 2), 0.0), axis=0)[0:LEVELS]


def per_device(row_devices, col_devices, surface_field, land_words):
    rows, cols = surface_field.shape
    f32 = jnp.float32
    levels = tuple(
        jax.ShapeDtypeStruct((rows >> level, cols >> level), f32) for level in range(1, LEVELS + 1)
    )
    scratch = [
        pltpu.VMEM((land_words.shape[1], rows), jnp.int32),
        pltpu.VMEM((cols // LANES, rows, LANES), f32),
        pltpu.VMEM((rows + 2 * HALO, LANES), jnp.int32),
        pltpu.VMEM((rows + 2 * HALO, LANES), f32),
        pltpu.VMEM((2 * HALO, rows), f32),
        pltpu.VMEM((2 * HALO, rows), f32),
        pltpu.VMEM((2 * HALO, rows + 2 * LANES), f32),
        pltpu.VMEM((2 * HALO, rows + 2 * LANES), f32),
        pltpu.VMEM((HALO, cols), f32),
        pltpu.VMEM((HALO, cols), f32),
        pltpu.VMEM((land_words.shape[1], LANES), jnp.int32),
        pltpu.VMEM((land_words.shape[1], LANES), jnp.int32),
    ]
    for level in range(LEVELS):
        shape = ((cols >> level) // LANES + 2, (rows >> level) + 48, LANES)
        scratch += [pltpu.VMEM(shape, f32)] * 2
    others = row_devices * col_devices - 1
    scratch += [
        pltpu.VMEM((4 * (rows // 2 + 16), cols + 2 * LANES), jnp.bfloat16),
        pltpu.VMEM((8, LANES), f32),
        pltpu.VMEM((others, LANES), f32),
        pltpu.SemaphoreType.DMA((cols // LANES,)),
        pltpu.SemaphoreType.DMA,
        pltpu.SemaphoreType.DMA((10,)),
        pltpu.SemaphoreType.DMA((10,)),
        pltpu.SemaphoreType.DMA((others,)),
        pltpu.SemaphoreType.DMA((others,)),
    ]
    vmem = pl.BlockSpec(memory_space=pltpu.VMEM)
    small = jax.ShapeDtypeStruct((LEVELS,), f32)
    found = pl.pallas_call(
        functools.partial(kernel, row_devices, col_devices),
        out_shape=tuple(pltpu.VMEM(each.shape, each.dtype) for each in (*levels, small, small)),
        in_specs=[pl.BlockSpec(memory_space=pltpu.HBM)] * 2,
        out_specs=(vmem,) * (LEVELS + 2),
        scratch_shapes=scratch,
        compiler_params=pltpu.CompilerParams(
            collective_id=0, has_side_effects=True, vmem_limit_bytes=56 * 1024 * 1024
        ),
        name="coarsen_levels",
    )(surface_field, land_words.T)

    any_place = pl.BlockSpec(memory_space=pl.ANY)
    return pl.pallas_call(
        hand_over,
        out_shape=(*levels, small, small),
        in_specs=[vmem] * (LEVELS + 2),
        out_specs=(any_place,) * (LEVELS + 2),
        scratch_shapes=[pltpu.SemaphoreType.DMA((LEVELS + 2,))],
        compiler_params=pltpu.CompilerParams(vmem_limit_bytes=8 * 1024 * 1024),
        name="hand_over",
    )(*found)


def hand_over(*refs):
    count = LEVELS + 2
    sources, targets, sems = refs[:count], refs[count : 2 * count], refs[2 * count]
    copies = [
        pltpu.make_async_copy(sources[at], targets[at], sems.at[at]) for at in range(count)
    ]
    for copy in copies:
        copy.start()
    for copy in copies:
        copy.wait()


def solution(mesh):
    return jax.shard_map(
        functools.partial(per_device, mesh.shape["rows"], mesh.shape["cols"]),
        mesh=mesh,
        in_specs=(P("rows", "cols"), P("rows", "cols")),
        out_specs=(
            P("rows", "cols"),
            P("rows", "cols"),
            P("rows", "cols"),
            P("rows", "cols"),
            P(),
            P(),
        ),
        check_vma=False,
    )
```

```python
import functools
import math

import jax
import jax.numpy as jnp
from jax import lax
from jax.experimental import pallas as pl
from jax.experimental.pallas import tpu as pltpu
from jax.sharding import PartitionSpec as P

stencil_weights = (0.125, 0.375, 0.375, 0.125)
floor_value = 0.05
mean_eps = 1e-06
LEVELS = 4
LANES = 128
HALO = 16
EDGE = 16
MESH = pl.DeviceIdType.MESH
f32 = jnp.float32
bf16 = jnp.bfloat16


def kernel(
    row_devices,
    col_devices,
    field,
    land_words,
    level_one,
    level_two,
    level_three,
    level_four,
    means_ref,
    maxima_ref,
    fine,
    land,
    words,
    cosines,
    cos_rows,
    send_left,
    send_right,
    side,
    side_words,
    p0,
    c0,
    p1,
    c1,
    p2,
    c2,
    p3,
    c3,
    split0,
    edge0,
    split1,
    split2,
    split3,
    stat_own,
    stat_all,
    load_sem,
    land_sem,
    halo_send,
    halo_recv,
    stat_send,
    stat_recv,
):
    rows, cols = field.shape
    tiles = cols // LANES
    count_words = land.shape[0]
    row_at = lax.axis_index("rows")
    col_at = lax.axis_index("cols")
    total_rows = rows * row_devices
    has_above = row_at > 0
    has_below = row_at < row_devices - 1

    def device(down, right):
        return (
            lax.rem(row_at + down + row_devices, row_devices),
            lax.rem(col_at + right + col_devices, col_devices),
        )

    others = [
        (down, right)
        for down in range(row_devices)
        for right in range(col_devices)
        if (down, right) != (0, 0)
    ]

    barrier = pltpu.get_barrier_semaphore()
    for down, right in others:
        pl.semaphore_signal(barrier, inc=1, device_id=device(down, right), device_id_type=MESH)

    land_load = pltpu.make_async_copy(land_words, land, land_sem)
    land_load.start()

    def load(tile):
        start = tile * LANES
        if not isinstance(tile, int):
            start = pl.multiple_of(start, LANES)
        return pltpu.make_async_copy(
            field.at[:, pl.ds(start, LANES)],
            fine.at[tile, pl.ds(HALO, rows), :],
            load_sem.at[tile],
        )

    order = [0, tiles - 1, *range(1, tiles - 1)]
    for tile in order:
        load(tile).start()

    def clear(row_start, lane_start):
        fine[:, row_start : row_start + HALO, :] = jnp.zeros((tiles, HALO, LANES), f32)
        words[row_start : row_start + HALO, :] = jnp.zeros((HALO, LANES), jnp.int32)
        here = slice(lane_start, lane_start + LANES)
        side[0:HALO, here] = jnp.zeros((HALO, LANES), f32)
        side[LANES - HALO :, here] = jnp.zeros((HALO, LANES), f32)
        side_words[:, here] = jnp.zeros((8, LANES), jnp.int32)

    @pl.when(jnp.logical_not(has_above))
    def _():
        clear(0, 0)

    @pl.when(jnp.logical_not(has_below))
    def _():
        clear(HALO + rows, LANES + rows)

    land_load.wait()
    upright = land[...]
    if count_words < LANES:
        filler = jnp.zeros((LANES - count_words, rows), jnp.int32)
        upright = jnp.concatenate([upright, filler], axis=0)
    words[HALO : HALO + rows, :] = jnp.transpose(upright)

    load(0).wait()
    send_left[...] = jnp.transpose(fine[0, HALO : HALO + rows, :])[0:HALO, :]
    load(tiles - 1).wait()
    send_right[...] = jnp.transpose(fine[tiles - 1, HALO : HALO + rows, :])[LANES - HALO :, :]
    for tile in range(1, tiles - 1):
        load(tile).wait()

    pl.semaphore_wait(barrier, len(others))

    first_words = land.at[0:1, :]
    last_words = land.at[count_words - 1 : count_words, :]
    own_lanes = pl.ds(LANES, rows)
    top_lanes = pl.ds(0, LANES)
    bottom_lanes = pl.ds(LANES + rows, LANES)
    ahead = pl.ds(0, LANES)
    behind = pl.ds(rows - LANES, LANES)
    right_side = side.at[0:HALO, :]
    left_side = side.at[LANES - HALO :, :]
    right_words = side_words.at[0:1, :]
    left_words = side_words.at[1:2, :]
    across_plan = (
        (send_left, right_side.at[:, own_lanes], (0, -1)),
        (send_right, left_side.at[:, own_lanes], (0, 1)),
        (first_words, right_words.at[:, own_lanes], (0, -1)),
        (last_words, left_words.at[:, own_lanes], (0, 1)),
    )
    down_plan = (
        (fine.at[:, rows : rows + HALO, :], fine.at[:, 0:HALO, :], (1, 0)),
        (words.at[rows : rows + HALO, :], words.at[0:HALO, :], (1, 0)),
        (send_left.at[:, behind], right_side.at[:, top_lanes], (1, -1)),
        (send_right.at[:, behind], left_side.at[:, top_lanes], (1, 1)),
        (first_words.at[:, behind], right_words.at[:, top_lanes], (1, -1)),
        (last_words.at[:, behind], left_words.at[:, top_lanes], (1, 1)),
    )
    up_plan = (
        (fine.at[:, HALO : 2 * HALO, :], fine.at[:, HALO + rows :, :], (-1, 0)),
        (words.at[HALO : 2 * HALO, :], words.at[HALO + rows :, :], (-1, 0)),
        (send_left.at[:, ahead], right_side.at[:, bottom_lanes], (-1, -1)),
        (send_right.at[:, ahead], left_side.at[:, bottom_lanes], (-1, 1)),
        (first_words.at[:, ahead], right_words.at[:, bottom_lanes], (-1, -1)),
        (last_words.at[:, ahead], left_words.at[:, bottom_lanes], (-1, 1)),
    )
    plans = (across_plan, down_plan, up_plan)
    first_slot = (0, len(across_plan), len(across_plan) + len(down_plan))

    def copies(which):
        return [
            pltpu.make_async_remote_copy(
                src_ref=source,
                dst_ref=target,
                send_sem=halo_send.at[first_slot[which] + place],
                recv_sem=halo_recv.at[first_slot[which] + place],
                device_id=device(down, right),
                device_id_type=MESH,
            )
            for place, (source, target, (down, right)) in enumerate(plans[which])
        ]

    for copy in copies(0):
        copy.start()

    @pl.when(has_below)
    def _():
        for copy in copies(1):
            copy.start()

    @pl.when(has_above)
    def _():
        for copy in copies(2):
            copy.start()

    blocks = rows // LANES + 2
    packed = cos_rows.shape
    row_index = (
        row_at * rows
        - LANES
        + lax.broadcasted_iota(jnp.int32, packed, 0) * LANES
        + lax.broadcasted_iota(jnp.int32, packed, 1)
    )
    latitude = ((row_index.astype(f32) + 0.5) / total_rows - 0.5) * math.pi
    on_globe = jnp.logical_and(row_index >= 0, row_index < total_rows)
    cos_rows[...] = jnp.where(on_globe, jnp.cos(latitude), 0.0)

    def placed(block):
        if block == 0:
            return slice(LANES - HALO, LANES), 0
        if block == blocks - 1:
            return slice(0, HALO), HALO + rows
        return slice(0, LANES), HALO + (block - 1) * LANES

    for block in range(blocks):
        taken, at = placed(block)
        spread = jnp.broadcast_to(cos_rows[block : block + 1, :], (LANES, LANES))
        cosines[at : at + taken.stop - taken.start, :] = jnp.transpose(spread)[taken, :]

    for product, cover, width in ((p0, c0, 8), (p1, c1, 16), (p2, c2, 16), (p3, c3, 16)):
        for ref in (product, cover):
            shape = (ref.shape[0], width, LANES)
            ref[:, 0:width, :] = jnp.zeros(shape, f32)
            ref[:, ref.shape[1] - width :, :] = jnp.zeros(shape, f32)

    def decode(tile, start, count):
        lanes = lax.broadcasted_iota(jnp.int32, (count, LANES), 1)
        place = tile * (LANES // 32) + lax.shift_right_logical(lanes, 5)
        word = jnp.take_along_axis(
            words[pl.ds(start, count), :], place, axis=1, mode="promise_in_bounds"
        )
        bit = lax.shift_left(jnp.ones_like(lanes), jnp.bitwise_and(lanes, 31))
        cover = jnp.where(
            jnp.bitwise_and(word, bit) != 0, cosines[pl.ds(start, count), :], 0.0
        )
        c0[tile, pl.ds(8 + start, count), :] = cover
        p0[tile, pl.ds(8 + start, count), :] = cover * fine[tile, pl.ds(start, count), :]

    sources = ((p0, c0), (p1, c1), (p2, c2), (p3, c3))
    outputs = (level_one, level_two, level_three, level_four)

    def downward(level, tile, first, count, target, at, stride, lanes_at):
        for place, ref in enumerate(sources[level]):
            taps = [ref[tile, pl.ds(7 + a + 2 * first, count, stride=2), :] for a in range(4)]
            down = (taps[0] + taps[3]) + 3.0 * (taps[1] + taps[2])
            high = down.astype(bf16)
            low = (down - high.astype(f32)).astype(bf16)
            for lane_at in lanes_at:
                where = pl.ds(lane_at, LANES)
                target[pl.ds(2 * place * stride + at, count), where] = high
                target[pl.ds((2 * place + 1) * stride + at, count), where] = low

    band_row = lax.broadcasted_iota(jnp.int32, (4 * LANES, LANES), 0)
    band_col = lax.broadcasted_iota(jnp.int32, (4 * LANES, LANES), 1)
    tap = band_row - (LANES - 1) - 2 * band_col
    band = jnp.where(
        jnp.logical_or(tap == 0, tap == 3),
        stencil_weights[0] / 8.0,
        jnp.where(jnp.logical_or(tap == 1, tap == 2), stencil_weights[1] / 8.0, 0.0),
    )
    right_band = jnp.where(band_col < LANES // 2, band, 0.0)[: 2 * LANES].astype(bf16)
    left_band = jnp.where(band_col >= LANES // 2, band, 0.0)[2 * LANES :].astype(bf16)
    band = band.astype(bf16)

    def across(source, count, parts):
        result = None
        for start, table in parts:
            part = jnp.dot(
                source[0 : 4 * count, pl.ds(start, table.shape[0])],
                table,
                preferred_element_type=f32,
            )
            result = part if result is None else result + part
        num = result[0:count] + result[count : 2 * count]
        den = result[2 * count : 3 * count] + result[3 * count :]
        return num / jnp.maximum(den, floor_value), den

    def own_parts(tile):
        start = tile * 2 * LANES
        if not isinstance(tile, int):
            start = pl.multiple_of(start, 2 * LANES)
        return ((start, band),)

    def side_parts(tiles_in):
        return ((tiles_in * LANES, right_band), (0, left_band))

    def tally(stat, value, cover, product):
        def parts(array):
            return array.reshape(array.shape[0] // 8, 8, LANES)

        weighted, total, largest = stat
        return (
            weighted + jnp.sum(parts(product), axis=0),
            total + jnp.sum(parts(cover), axis=0),
            jnp.maximum(largest, jnp.max(parts(value), axis=0)),
        )

    zero = jnp.zeros((8, LANES), f32)
    fresh = (zero, zero, jnp.full((8, LANES), -jnp.inf, f32))
    above_factor = jnp.where(has_above, 1.0, 0.0).astype(f32)
    below_factor = jnp.where(has_below, 1.0, 0.0).astype(f32)

    own = rows // 2
    inner = own + 2 * 8 - 2 * EDGE
    tiles_out = tiles // 2

    @pl.loop(0, tiles)
    def _(tile):
        for start in range(0, rows, 64):
            decode(tile, HALO + start, 64)
        lane_at = pl.multiple_of((tile + 1) * LANES, LANES)
        downward(0, tile, EDGE, inner, split0, 0, inner, (lane_at,))

    def inner_columns(tile, stat):
        value, cover = across(split0, inner, own_parts(tile))
        product = cover * value
        if isinstance(tile, int):
            lanes = slice(tile * LANES, (tile + 1) * LANES)
        else:
            lanes = pl.ds(pl.multiple_of(tile * LANES, LANES), LANES)
        p1[tile, 16 + EDGE : 16 + EDGE + inner, :] = product
        c1[tile, 16 + EDGE : 16 + EDGE + inner, :] = cover
        level_one[EDGE - 8 : EDGE - 8 + inner, lanes] = value
        return tally(stat, value, cover, product)

    stat = lax.fori_loop(1, tiles_out - 1, inner_columns, fresh)

    for copy in copies(0):
        copy.wait()

    @pl.when(has_below)
    def _():
        for copy in copies(1):
            copy.wait_send()
        for copy in copies(2):
            copy.wait_recv()

    @pl.when(has_above)
    def _():
        for copy in copies(2):
            copy.wait_send()
        for copy in copies(1):
            copy.wait_recv()

    sub = lax.broadcasted_iota(jnp.int32, (HALO, LANES), 0)
    for block in range(blocks):
        here = slice(block * LANES, (block + 1) * LANES)
        turn = jnp.broadcast_to(cos_rows[block : block + 1, :], (HALO, LANES))
        pieces = []
        for index, (at, shift) in enumerate(((0, 0), (LANES - HALO, 32 - HALO))):
            word = jnp.broadcast_to(side_words[index : index + 1, here], (HALO, LANES))
            flag = jnp.bitwise_and(lax.shift_right_logical(word, sub + shift), 1)
            cover = jnp.where(flag != 0, turn, 0.0)
            pieces.append((cover, cover * side[at : at + HALO, here]))
        filler = jnp.zeros((LANES - 2 * HALO, LANES), f32)
        taken, at = placed(block)
        size = taken.stop - taken.start
        for kind, ref in ((0, c0), (1, p0)):
            flat = jnp.concatenate([pieces[0][kind], filler, pieces[1][kind]], axis=0)
            ref[tiles, 8 + at : 8 + at + size, :] = jnp.transpose(flat)[taken, :]

    for tile in range(tiles):
        decode(tile, 0, HALO)
        decode(tile, HALO + rows, HALO)

    ends = (0, (tiles + 1) * LANES)
    downward(0, tiles, EDGE, inner, split0, 0, inner, ends)
    for tile in range(tiles + 1):
        lanes_at = ends if tile == tiles else ((tile + 1) * LANES,)
        downward(0, tile, 0, EDGE, edge0, 0, 2 * EDGE, lanes_at)
        downward(0, tile, EDGE + inner, EDGE, edge0, EDGE, 2 * EDGE, lanes_at)

    stats = []
    stat = inner_columns(0, stat)
    stat = inner_columns(tiles_out - 1, stat)
    value, cover = across(split0, inner, side_parts(tiles))
    p1[tiles_out, 16 + EDGE : 16 + EDGE + inner, :] = cover * value
    c1[tiles_out, 16 + EDGE : 16 + EDGE + inner, :] = cover
    for tile in range(tiles_out + 1):
        parts = side_parts(tiles) if tile == tiles_out else own_parts(tile)
        value, cover = across(edge0, 2 * EDGE, parts)
        product = cover * value
        for ref, array in ((p1, product), (c1, cover)):
            ref[tile, 16:24, :] = array[0:8] * above_factor
            ref[tile, 24 : 16 + EDGE, :] = array[8:EDGE]
            ref[tile, 16 + EDGE + inner : 24 + own, :] = array[EDGE : 2 * EDGE - 8]
            ref[tile, 24 + own : 32 + own, :] = array[2 * EDGE - 8 :] * below_factor
        if tile < tiles_out:
            lanes = slice(tile * LANES, (tile + 1) * LANES)
            level_one[0 : EDGE - 8, lanes] = value[8:EDGE]
            level_one[own - EDGE + 8 :, lanes] = value[EDGE : 2 * EDGE - 8]
            middle = slice(8, 2 * EDGE - 8)
            stat = tally(stat, value[middle], cover[middle], product[middle])
    stats.append(stat)

    splits = (None, split1, split2, split3)
    for level in range(1, LEVELS):
        source, output = splits[level], outputs[level]
        own = output.shape[0]
        last = level + 1 == LEVELS
        first = 8 if last else 0
        count = own if last else own + 16
        tiles_in = sources[level][0].shape[0] - 1
        tiles_out = output.shape[1] // LANES
        for tile in range(tiles_in + 1):
            lanes_at = (0, (tiles_in + 1) * LANES) if tile == tiles_in else ((tile + 1) * LANES,)
            downward(level, tile, first, count, source, 0, count, lanes_at)
        stat = fresh
        for tile in range(tiles_out + (not last)):
            parts = side_parts(tiles_in) if tile == tiles_out else own_parts(tile)
            value, cover = across(source, count, parts)
            product = cover * value
            middle = slice(8 - first, 8 - first + own)
            if not last:
                for ref, array in zip(sources[level + 1], (product, cover)):
                    ref[tile, 16:24, :] = array[0:8] * above_factor
                    ref[tile, 24 : 24 + own, :] = array[middle]
                    ref[tile, 24 + own : 32 + own, :] = array[8 + own :] * below_factor
            if tile < tiles_out:
                output[:, tile * LANES : (tile + 1) * LANES] = value[middle]
                stat = tally(stat, value[middle], cover[middle], product[middle])
        stats.append(stat)

    lane = lax.broadcasted_iota(jnp.int32, (8, LANES), 1)
    row = lax.broadcasted_iota(jnp.int32, (8, LANES), 0)
    mine = jnp.zeros((8, LANES), f32)
    for kind, reduce in ((0, jnp.sum), (1, jnp.sum), (2, jnp.max)):
        tile = jnp.zeros((8, LANES), f32)
        for level in range(LEVELS):
            tile = jnp.where(row == level, reduce(stats[level][kind], axis=0, keepdims=True), tile)
        mine = jnp.where(lane == row + kind * LEVELS, reduce(tile, axis=1, keepdims=True), mine)
    mine = jnp.where(row < LEVELS, mine, 0.0)
    stat_own[...] = jnp.broadcast_to(jnp.sum(mine, axis=0, keepdims=True), (8, LANES))
    sends = []
    for place, (down, right) in enumerate(others):
        copy = pltpu.make_async_remote_copy(
            src_ref=stat_own.at[0:1],
            dst_ref=stat_all.at[place : place + 1],
            send_sem=stat_send.at[place],
            recv_sem=stat_recv.at[place],
            device_id=device(down, right),
            device_id_type=MESH,
        )
        copy.start()
        sends.append(copy)
    for copy in sends:
        copy.wait()
    first = stat_own[0:1, :]
    summed = first + jnp.sum(stat_all[...], axis=0, keepdims=True)
    largest = jnp.maximum(first, jnp.max(stat_all[...], axis=0, keepdims=True))
    summed = jnp.broadcast_to(summed, (8, LANES))
    largest = jnp.broadcast_to(largest, (8, LANES))

    def pick(array, kind):
        here = jnp.logical_and(lane == row + kind * LEVELS, row < LEVELS)
        return jnp.sum(jnp.where(here, array, 0.0), axis=1, keepdims=True)

    level_means = pick(summed, 0) / (pick(summed, 1) + mean_eps)
    diagonal = jnp.logical_and(lane == row, row < LEVELS)
    means_ref[...] = jnp.sum(jnp.where(diagonal, level_means, 0.0), axis=0)[0:LEVELS]
    maxima_ref[...] = jnp.sum(jnp.where(diagonal, pick(largest, 2), 0.0), axis=0)[0:LEVELS]


def per_device(row_devices, col_devices, surface_field, land_words):
    rows, cols = surface_field.shape
    tiles = cols // LANES
    levels = tuple(
        jax.ShapeDtypeStruct((rows >> level, cols >> level), f32) for level in range(1, LEVELS + 1)
    )
    blocks = rows // LANES + 2
    scratch = [
        pltpu.VMEM((tiles, rows + 2 * HALO, LANES), f32),
        pltpu.VMEM((land_words.shape[1], rows), jnp.int32),
        pltpu.VMEM((rows + 2 * HALO, LANES), jnp.int32),
        pltpu.VMEM((rows + 2 * HALO, LANES), f32),
        pltpu.VMEM((8 * (-(-blocks // 8)), LANES), f32),
        pltpu.VMEM((HALO, rows), f32),
        pltpu.VMEM((HALO, rows), f32),
        pltpu.VMEM((LANES, rows + 2 * LANES), f32),
        pltpu.VMEM((8, rows + 2 * LANES), jnp.int32),
    ]
    for level in range(LEVELS):
        shape = ((cols >> level) // LANES + 1, (rows >> level) + 48, LANES)
        scratch += [pltpu.VMEM(shape, f32)] * 2
    scratch += [
        pltpu.VMEM((4 * (rows // 2 + 16 - 2 * EDGE), cols + 2 * LANES), bf16),
        pltpu.VMEM((8 * EDGE, cols + 2 * LANES), bf16),
    ]
    for level in range(1, LEVELS):
        margin = 16 if level + 1 < LEVELS else 0
        shape = (4 * ((rows >> (level + 1)) + margin), (cols >> level) + 2 * LANES)
        scratch.append(pltpu.VMEM(shape, bf16))
    others = row_devices * col_devices - 1
    scratch += [
        pltpu.VMEM((8, LANES), f32),
        pltpu.VMEM((others, LANES), f32),
        pltpu.SemaphoreType.DMA((tiles,)),
        pltpu.SemaphoreType.DMA,
        pltpu.SemaphoreType.DMA((16,)),
        pltpu.SemaphoreType.DMA((16,)),
        pltpu.SemaphoreType.DMA((others,)),
        pltpu.SemaphoreType.DMA((others,)),
    ]
    vmem = pl.BlockSpec(memory_space=pltpu.VMEM)
    small = jax.ShapeDtypeStruct((LEVELS,), f32)
    results = (*levels, small, small)
    found = pl.pallas_call(
        functools.partial(kernel, row_devices, col_devices),
        out_shape=tuple(pltpu.VMEM(each.shape, each.dtype) for each in results),
        in_specs=[pl.BlockSpec(memory_space=pltpu.HBM)] * 2,
        out_specs=(vmem,) * len(results),
        scratch_shapes=scratch,
        compiler_params=pltpu.CompilerParams(
            collective_id=0, has_side_effects=True, vmem_limit_bytes=56 * 1024 * 1024
        ),
        name="coarsen_levels",
    )(surface_field, land_words.T)

    return pl.pallas_call(
        hand_over,
        out_shape=results,
        in_specs=[vmem] * len(results),
        out_specs=(pl.BlockSpec(memory_space=pl.ANY),) * len(results),
        scratch_shapes=[pltpu.SemaphoreType.DMA((len(results),))],
        compiler_params=pltpu.CompilerParams(vmem_limit_bytes=8 * 1024 * 1024),
        name="hand_over",
    )(*found)


def hand_over(*refs):
    count = LEVELS + 2
    sources, targets, sems = refs[:count], refs[count : 2 * count], refs[2 * count]
    copies = [
        pltpu.make_async_copy(sources[at], targets[at], sems.at[at]) for at in range(count)
    ]
    for copy in copies:
        copy.start()
    for copy in copies:
        copy.wait()


def solution(mesh):
    return jax.shard_map(
        functools.partial(per_device, mesh.shape["rows"], mesh.shape["cols"]),
        mesh=mesh,
        in_specs=(P("rows", "cols"), P("rows", "cols")),
        out_specs=(P("rows", "cols"),) * LEVELS + (P(), P()),
        check_vma=False,
    )
```

```python
import functools
import math

import jax
import jax.numpy as jnp
from jax import lax
from jax.experimental import pallas as pl
from jax.experimental.pallas import tpu as pltpu
from jax.sharding import PartitionSpec as P

stencil_weights = (0.125, 0.375, 0.375, 0.125)
floor_value = 0.05
mean_eps = 1e-06
LEVELS = 4
LANES = 128
HALO = 16
EDGE = 16
MESH = pl.DeviceIdType.MESH
f32 = jnp.float32
bf16 = jnp.bfloat16


def kernel(
    row_devices,
    col_devices,
    field,
    land_words,
    level_one,
    level_two,
    level_three,
    level_four,
    means_ref,
    maxima_ref,
    fine,
    land,
    words,
    cosines,
    cos_rows,
    send_left,
    send_right,
    side,
    side_words,
    p0,
    c0,
    p1,
    c1,
    p2,
    c2,
    p3,
    c3,
    split0,
    split1,
    split2,
    split3,
    edge0,
    edge1,
    edge2,
    edge3,
    partial0,
    partial1,
    partial2,
    partial3,
    stat_own,
    stat_all,
    load_sem,
    land_sem,
    halo_send,
    halo_recv,
    stat_send,
    stat_recv,
):
    rows, cols = field.shape
    tiles = cols // LANES
    count_words = land.shape[0]
    row_at = lax.axis_index("rows")
    col_at = lax.axis_index("cols")
    total_rows = rows * row_devices
    has_above = row_at > 0
    has_below = row_at < row_devices - 1

    def device(down, right):
        return (
            lax.rem(row_at + down + row_devices, row_devices),
            lax.rem(col_at + right + col_devices, col_devices),
        )

    others = [
        (down, right)
        for down in range(row_devices)
        for right in range(col_devices)
        if (down, right) != (0, 0)
    ]

    barrier = pltpu.get_barrier_semaphore()
    for down, right in others:
        pl.semaphore_signal(barrier, inc=1, device_id=device(down, right), device_id_type=MESH)

    land_load = pltpu.make_async_copy(land_words, land, land_sem)
    land_load.start()

    def load(tile):
        start = tile * LANES
        if not isinstance(tile, int):
            start = pl.multiple_of(start, LANES)
        return pltpu.make_async_copy(
            field.at[:, pl.ds(start, LANES)],
            fine.at[tile, pl.ds(HALO, rows), :],
            load_sem.at[0 if tile == 0 else 2 if tile < tiles - 1 else 1],
        )

    def settle(ref, sem):
        pltpu.make_async_copy(ref, ref, sem).wait()

    order = [0, tiles - 1, *range(1, tiles - 1)]
    for tile in order:
        load(tile).start()

    def clear(row_start, lane_start):
        fine[:, row_start : row_start + HALO, :] = jnp.zeros((tiles, HALO, LANES), f32)
        words[row_start : row_start + HALO, :] = jnp.zeros((HALO, LANES), jnp.int32)
        here = slice(lane_start, lane_start + LANES)
        side[0:HALO, here] = jnp.zeros((HALO, LANES), f32)
        side[LANES - HALO :, here] = jnp.zeros((HALO, LANES), f32)
        side_words[:, here] = jnp.zeros((8, LANES), jnp.int32)

    @pl.when(jnp.logical_not(has_above))
    def _():
        clear(0, 0)

    @pl.when(jnp.logical_not(has_below))
    def _():
        clear(HALO + rows, LANES + rows)

    land_load.wait()
    upright = land[...]
    if count_words < LANES:
        filler = jnp.zeros((LANES - count_words, rows), jnp.int32)
        upright = jnp.concatenate([upright, filler], axis=0)
    words[HALO : HALO + rows, :] = jnp.transpose(upright)

    load(0).wait()
    send_left[...] = jnp.transpose(fine[0, HALO : HALO + rows, :])[0:HALO, :]
    load(tiles - 1).wait()
    send_right[...] = jnp.transpose(fine[tiles - 1, HALO : HALO + rows, :])[LANES - HALO :, :]
    settle(fine.at[1 : tiles - 1, HALO : HALO + rows, :], load_sem.at[2])

    pl.semaphore_wait(barrier, len(others))

    first_words = land.at[0:1, :]
    last_words = land.at[count_words - 1 : count_words, :]
    own_lanes = pl.ds(LANES, rows)
    top_lanes = pl.ds(0, LANES)
    bottom_lanes = pl.ds(LANES + rows, LANES)
    ahead = pl.ds(0, LANES)
    behind = pl.ds(rows - LANES, LANES)
    right_side = side.at[0:HALO, :]
    left_side = side.at[LANES - HALO :, :]
    right_words = side_words.at[0:1, :]
    left_words = side_words.at[1:2, :]
    across_plan = (
        (send_left, right_side.at[:, own_lanes], (0, -1)),
        (send_right, left_side.at[:, own_lanes], (0, 1)),
        (first_words, right_words.at[:, own_lanes], (0, -1)),
        (last_words, left_words.at[:, own_lanes], (0, 1)),
    )
    down_plan = (
        (fine.at[:, rows : rows + HALO, :], fine.at[:, 0:HALO, :], (1, 0)),
        (words.at[rows : rows + HALO, :], words.at[0:HALO, :], (1, 0)),
        (send_left.at[:, behind], right_side.at[:, top_lanes], (1, -1)),
        (send_right.at[:, behind], left_side.at[:, top_lanes], (1, 1)),
    )
    down_words_plan = (
        (first_words.at[:, behind], right_words.at[:, top_lanes], (1, -1)),
        (last_words.at[:, behind], left_words.at[:, top_lanes], (1, 1)),
    )
    up_plan = (
        (fine.at[:, HALO : 2 * HALO, :], fine.at[:, HALO + rows :, :], (-1, 0)),
        (words.at[HALO : 2 * HALO, :], words.at[HALO + rows :, :], (-1, 0)),
        (send_left.at[:, ahead], right_side.at[:, bottom_lanes], (-1, -1)),
        (send_right.at[:, ahead], left_side.at[:, bottom_lanes], (-1, 1)),
    )
    up_words_plan = (
        (first_words.at[:, ahead], right_words.at[:, bottom_lanes], (-1, -1)),
        (last_words.at[:, ahead], left_words.at[:, bottom_lanes], (-1, 1)),
    )
    plans = (across_plan, down_plan, up_plan, down_words_plan, up_words_plan)
    downs, ups = (1, 3), (2, 4)

    def settle_halo(which, sem):
        moved = sum(math.prod(source.shape) for source, _, _ in plans[which])
        if moved % (8 * LANES):
            settle(side_words.at[0:1, 0:moved], sem.at[which])
        else:
            settle(fine.at[0, 0 : moved // LANES, :], sem.at[which])

    def copies(which):
        return [
            pltpu.make_async_remote_copy(
                src_ref=source,
                dst_ref=target,
                send_sem=halo_send.at[which],
                recv_sem=halo_recv.at[which],
                device_id=device(down, right),
                device_id_type=MESH,
            )
            for source, target, (down, right) in plans[which]
        ]

    for copy in copies(0):
        copy.start()

    @pl.when(has_below)
    def _():
        for which in downs:
            for copy in copies(which):
                copy.start()

    @pl.when(has_above)
    def _():
        for which in ups:
            for copy in copies(which):
                copy.start()

    blocks = rows // LANES + 2
    packed = cos_rows.shape
    row_index = (
        row_at * rows
        - LANES
        + lax.broadcasted_iota(jnp.int32, packed, 0) * LANES
        + lax.broadcasted_iota(jnp.int32, packed, 1)
    )
    latitude = ((row_index.astype(f32) + 0.5) / total_rows - 0.5) * math.pi
    on_globe = jnp.logical_and(row_index >= 0, row_index < total_rows)
    cos_rows[...] = jnp.where(on_globe, jnp.cos(latitude), 0.0)

    def placed(block):
        if block == 0:
            return slice(LANES - HALO, LANES), 0
        if block == blocks - 1:
            return slice(0, HALO), HALO + rows
        return slice(0, LANES), HALO + (block - 1) * LANES

    for block in range(blocks):
        taken, at = placed(block)
        spread = jnp.broadcast_to(cos_rows[block : block + 1, :], (LANES, LANES))
        cosines[at : at + taken.stop - taken.start, :] = jnp.transpose(spread)[taken, :]

    for product, cover, width in ((p0, c0, 8), (p1, c1, 16), (p2, c2, 16), (p3, c3, 16)):
        for ref in (product, cover):
            shape = (ref.shape[0], width, LANES)
            ref[:, 0:width, :] = jnp.zeros(shape, f32)
            ref[:, ref.shape[1] - width :, :] = jnp.zeros(shape, f32)

    def decode(tile, start, count):
        lanes = lax.broadcasted_iota(jnp.int32, (count, LANES), 1)
        place = tile * (LANES // 32) + lax.shift_right_logical(lanes, 5)
        word = jnp.take_along_axis(
            words[pl.ds(start, count), :], place, axis=1, mode="promise_in_bounds"
        )
        bit = lax.shift_left(jnp.ones_like(lanes), jnp.bitwise_and(lanes, 31))
        cover = jnp.where(
            jnp.bitwise_and(word, bit) != 0, cosines[pl.ds(start, count), :], 0.0
        )
        c0[tile, pl.ds(8 + start, count), :] = cover
        p0[tile, pl.ds(8 + start, count), :] = cover * fine[tile, pl.ds(start, count), :]

    sources = ((p0, c0), (p1, c1), (p2, c2), (p3, c3))
    splits = (split0, split1, split2, split3)
    edges = (edge0, edge1, edge2, edge3)
    partials = (partial0, partial1, partial2, partial3)
    outputs = (level_one, level_two, level_three, level_four)

    def downward(level, tile, first, count, target, at, stride):
        lanes = pl.ds(tile * LANES, LANES)
        for place, ref in enumerate(sources[level]):
            taps = [ref[tile, pl.ds(7 + a + 2 * first, count, stride=2), :] for a in range(4)]
            down = (taps[0] + taps[3]) + 3.0 * (taps[1] + taps[2])
            high = down.astype(bf16)
            low = (down - high.astype(f32)).astype(bf16)
            target[pl.ds(2 * place * stride + at, count), lanes] = high
            target[pl.ds((2 * place + 1) * stride + at, count), lanes] = low

    def table(tap, keep=True):
        weight = jnp.where(
            jnp.logical_or(tap == 0, tap == 3),
            stencil_weights[0] / 8.0,
            jnp.where(jnp.logical_or(tap == 1, tap == 2), stencil_weights[1] / 8.0, 0.0),
        )
        return jnp.where(keep, weight, 0.0).astype(bf16)

    band_row = lax.broadcasted_iota(jnp.int32, (4 * LANES, LANES), 0)
    band_col = lax.broadcasted_iota(jnp.int32, (4 * LANES, LANES), 1)
    band = table(band_row - (LANES - 1) - 2 * band_col)

    half = LANES // 2

    def column(at):
        middle = jnp.where(at == half, 0, -1)
        away = jnp.where(at > half, at - LANES, at)
        return jnp.where(jnp.logical_or(at == half, at == half - 1), middle, away)

    lane_in = lax.broadcasted_iota(jnp.int32, (LANES, LANES), 0)
    lane_out = lax.broadcasted_iota(jnp.int32, (LANES, LANES), 1)
    leftward = lane_out >= half
    from_side = table(
        column(lane_in) - 2 * column(lane_out) + 1, (lane_in >= half) == leftward
    )
    from_first = table(lane_in - 2 * column(lane_out) + 1, leftward)
    from_last = table(lane_in - LANES - 2 * column(lane_out) + 1, jnp.logical_not(leftward))
    last_and_side = jnp.concatenate([from_last, from_side], axis=0)

    def across(source, count, parts):
        result = None
        for start, weights in parts:
            part = jnp.dot(
                source[0 : 4 * count, start * LANES : start * LANES + weights.shape[0]],
                weights,
                preferred_element_type=f32,
            )
            result = part if result is None else result + part
        num = result[0:count] + result[count : 2 * count]
        den = result[2 * count : 3 * count] + result[3 * count :]
        return num, den

    def own_parts(tile, tiles_in):
        start = max(2 * tile - 1, 0)
        stop = min(2 * tile + 3, tiles_in)
        skip = start - (2 * tile - 1)
        return ((start, band[skip * LANES : (skip + stop - start) * LANES]),)

    def finish(num, den):
        value = num / jnp.maximum(den, floor_value)
        return value, den, den * value

    def ring(shape, tile, count_tiles):
        lanes = lax.broadcasted_iota(jnp.int32, shape, 1)
        if tile == count_tiles:
            return jnp.logical_or(lanes == half, lanes == half - 1)
        here = None
        if tile == 0:
            here = lanes == 0
        if tile == count_tiles - 1:
            final = lanes == LANES - 1
            here = final if here is None else jnp.logical_or(here, final)
        return here

    def tally(stat, value, cover, product):
        def parts(array):
            return array.reshape(array.shape[0] // 8, 8, LANES)

        weighted, total, largest = stat
        return (
            weighted + jnp.sum(parts(product), axis=0),
            total + jnp.sum(parts(cover), axis=0),
            jnp.maximum(largest, jnp.max(parts(value), axis=0)),
        )

    def masked(level, tile, value, cover, product):
        count_tiles = outputs[level].shape[1] // LANES
        here = ring(value.shape, tile, count_tiles)
        if tile == count_tiles:
            inside = jnp.where(here, value, -jnp.inf)
            return cover, product, (inside, jnp.where(here, cover, 0.0), jnp.where(here, product, 0.0))
        if here is not None:
            value = jnp.where(here, -jnp.inf, value)
            cover = jnp.where(here, 0.0, cover)
            product = jnp.where(here, 0.0, product)
        return cover, product, (value, cover, product)

    zero = jnp.zeros((8, LANES), f32)
    stats = [(zero, zero, jnp.full((8, LANES), -jnp.inf, f32)) for _ in range(LEVELS)]
    above_factor = jnp.where(has_above, 1.0, 0.0).astype(f32)
    below_factor = jnp.where(has_below, 1.0, 0.0).astype(f32)

    def inner_rows(level):
        return outputs[level].shape[0] + 16 - 2 * EDGE

    def inner_tile(level, tile, num, den):
        inner = inner_rows(level)
        value, cover, product = finish(num, den)
        cover, product, counted = masked(level, tile, value, cover, product)
        if level + 1 < LEVELS:
            for ref, array in zip(sources[level + 1], (product, cover)):
                ref[tile, 16 + EDGE : 16 + EDGE + inner, :] = array
        stats[level] = tally(stats[level], *counted)
        return value

    for level in range(LEVELS):
        inner = inner_rows(level)
        tiles_in = sources[level][0].shape[0] - 1
        tiles_out = outputs[level].shape[1] // LANES

        def feed(tile):
            if level == 0:
                for start in range(0, rows, 64):
                    decode(tile, HALO + start, 64)
            downward(level, tile, EDGE, inner, splits[level], 0, inner)

        fed = 0
        for tile in range(tiles_out):
            while fed < min(2 * tile + 3, tiles_in):
                feed(fed)
                fed += 1
            value = inner_tile(
                level, tile, *across(splits[level], inner, own_parts(tile, tiles_in))
            )
            lanes = slice(tile * LANES, (tile + 1) * LANES)
            outputs[level][EDGE - 8 : EDGE - 8 + inner, lanes] = value
        num, den = across(splits[level], inner, ((0, from_first), (tiles_in - 1, from_last)))
        partials[level][0] = num
        partials[level][1] = den

    settle_halo(0, halo_recv)

    @pl.when(has_below)
    def _():
        for which in ups:
            settle_halo(which, halo_recv)

    @pl.when(has_above)
    def _():
        for which in downs:
            settle_halo(which, halo_recv)

    sub = lax.broadcasted_iota(jnp.int32, (HALO, LANES), 0)
    for block in range(blocks):
        here = slice(block * LANES, (block + 1) * LANES)
        turn = jnp.broadcast_to(cos_rows[block : block + 1, :], (HALO, LANES))
        pieces = []
        for index, (at, shift) in enumerate(((0, 0), (LANES - HALO, 32 - HALO))):
            word = jnp.broadcast_to(side_words[index : index + 1, here], (HALO, LANES))
            flag = jnp.bitwise_and(lax.shift_right_logical(word, sub + shift), 1)
            cover = jnp.where(flag != 0, turn, 0.0)
            pieces.append((cover, cover * side[at : at + HALO, here]))
        filler = jnp.zeros((LANES - 2 * HALO, LANES), f32)
        taken, at = placed(block)
        size = taken.stop - taken.start
        for kind, ref in ((0, c0), (1, p0)):
            flat = jnp.concatenate([pieces[0][kind], filler, pieces[1][kind]], axis=0)
            ref[tiles, 8 + at : 8 + at + size, :] = jnp.transpose(flat)[taken, :]

    for tile in range(tiles):
        decode(tile, 0, HALO)
        decode(tile, HALO + rows, HALO)

    ring_values = []
    for level in range(LEVELS):
        inner = inner_rows(level)
        output = outputs[level]
        own = output.shape[0]
        tiles_in = sources[level][0].shape[0] - 1
        tiles_out = output.shape[1] // LANES
        downward(level, tiles_in, EDGE, inner, splits[level], 0, inner)
        for tile in range(tiles_in + 1):
            downward(level, tile, 0, EDGE, edges[level], 0, 2 * EDGE)
            downward(level, tile, EDGE + inner, EDGE, edges[level], EDGE, 2 * EDGE)
        num, den = across(splits[level], inner, ((tiles_in, from_side),))
        inner_value = inner_tile(
            level, tiles_out, num + partials[level][0], den + partials[level][1]
        )
        for tile in range(tiles_out + 1):
            if tile == tiles_out:
                parts = ((tiles_in - 1, last_and_side), (0, from_first))
            else:
                parts = own_parts(tile, tiles_in)
            value, cover, product = finish(*across(edges[level], 2 * EDGE, parts))
            cover, product, counted = masked(level, tile, value, cover, product)
            if level + 1 < LEVELS:
                for ref, array in zip(sources[level + 1], (product, cover)):
                    ref[tile, 16:24, :] = array[0:8] * above_factor
                    ref[tile, 24 : 16 + EDGE, :] = array[8:EDGE]
                    ref[tile, 16 + EDGE + inner : 24 + own, :] = array[EDGE : 2 * EDGE - 8]
                    ref[tile, 24 + own : 32 + own, :] = array[2 * EDGE - 8 :] * below_factor
            middle = slice(8, 2 * EDGE - 8)
            stats[level] = tally(stats[level], *(array[middle] for array in counted))
            if tile < tiles_out:
                lanes = slice(tile * LANES, (tile + 1) * LANES)
                output[0 : EDGE - 8, lanes] = value[8:EDGE]
                output[own - EDGE + 8 :, lanes] = value[EDGE : 2 * EDGE - 8]
            else:
                ring_values.append((inner_value, value[middle]))

    lane = lax.broadcasted_iota(jnp.int32, (8, LANES), 1)
    row = lax.broadcasted_iota(jnp.int32, (8, LANES), 0)
    mine = zero
    for level, (weighted, total, largest) in enumerate(stats):
        weighted = jnp.sum(weighted, axis=0, keepdims=True)
        total = jnp.sum(total, axis=0, keepdims=True)
        sums = jnp.sum(jnp.where(row == 0, weighted, total), axis=1, keepdims=True)
        largest = jnp.max(largest, axis=0, keepdims=True)
        largest = jnp.max(jnp.broadcast_to(largest, (8, LANES)), axis=1, keepdims=True)
        mine = jnp.where(lane == level, jnp.where(row < 2, sums, largest), mine)
    stat_own[...] = mine
    for place, (down, right) in enumerate(others):
        copy = pltpu.make_async_remote_copy(
            src_ref=stat_own.at[0:4],
            dst_ref=stat_all.at[place, 0:4],
            send_sem=stat_send,
            recv_sem=stat_recv,
            device_id=device(down, right),
            device_id_type=MESH,
        )
        copy.start()

    for output, (inner_value, edge_value) in zip(outputs, ring_values):
        own, width = output.shape
        tiles_out = width // LANES
        for start, array in (
            (0, edge_value[0:8]),
            (8, inner_value),
            (own - 8, edge_value[8:16]),
        ):
            turned = pltpu.roll(array, half, axis=1)
            here = slice(start, start + array.shape[0])
            for tile in sorted({0, tiles_out - 1}):
                lanes = slice(tile * LANES, (tile + 1) * LANES)
                at_ring = ring(array.shape, tile, tiles_out)
                output[here, lanes] = jnp.where(at_ring, turned, output[here, lanes])

    settle_halo(0, halo_send)

    @pl.when(has_below)
    def _():
        for which in downs:
            settle_halo(which, halo_send)

    @pl.when(has_above)
    def _():
        for which in ups:
            settle_halo(which, halo_send)

    arrived = stat_all.at[:, 0:4, :]
    settle(arrived, stat_recv)

    def combine(reduce):
        parts = [stat_own[0:4, :]] + [stat_all[place, 0:4, :] for place in range(len(others))]
        while len(parts) > 1:
            pairs = [reduce(*pair) for pair in zip(parts[0::2], parts[1::2])]
            parts = pairs + parts[2 * len(pairs) :]
        return parts[0]

    summed, largest = combine(jnp.add), combine(jnp.maximum)
    means_ref[...] = jnp.sum(summed[0:1] / (summed[1:2] + mean_eps), axis=0)[0:LEVELS]
    maxima_ref[...] = jnp.sum(largest[2:3], axis=0)[0:LEVELS]
    settle(arrived, stat_send)


def per_device(row_devices, col_devices, surface_field, land_words):
    rows, cols = surface_field.shape
    tiles = cols // LANES
    levels = tuple(
        jax.ShapeDtypeStruct((rows >> level, cols >> level), f32) for level in range(1, LEVELS + 1)
    )
    blocks = rows // LANES + 2
    scratch = [
        pltpu.VMEM((tiles, rows + 2 * HALO, LANES), f32),
        pltpu.VMEM((land_words.shape[1], rows), jnp.int32),
        pltpu.VMEM((rows + 2 * HALO, LANES), jnp.int32),
        pltpu.VMEM((rows + 2 * HALO, LANES), f32),
        pltpu.VMEM((8 * (-(-blocks // 8)), LANES), f32),
        pltpu.VMEM((HALO, rows), f32),
        pltpu.VMEM((HALO, rows), f32),
        pltpu.VMEM((LANES, rows + 2 * LANES), f32),
        pltpu.VMEM((8, rows + 2 * LANES), jnp.int32),
    ]
    for level in range(LEVELS):
        shape = ((cols >> level) // LANES + 1, (rows >> level) + 48, LANES)
        scratch += [pltpu.VMEM(shape, f32)] * 2
    for level in range(LEVELS):
        inner = (rows >> (level + 1)) + 16 - 2 * EDGE
        scratch.append(pltpu.VMEM((4 * inner, (cols >> level) + LANES), bf16))
    for level in range(LEVELS):
        scratch.append(pltpu.VMEM((8 * EDGE, (cols >> level) + LANES), bf16))
    for level in range(LEVELS):
        inner = (rows >> (level + 1)) + 16 - 2 * EDGE
        scratch.append(pltpu.VMEM((2, inner, LANES), f32))
    others = row_devices * col_devices - 1
    scratch += [
        pltpu.VMEM((8, LANES), f32),
        pltpu.VMEM((others, 8, LANES), f32),
        pltpu.SemaphoreType.DMA((3,)),
        pltpu.SemaphoreType.DMA,
        pltpu.SemaphoreType.DMA((5,)),
        pltpu.SemaphoreType.DMA((5,)),
        pltpu.SemaphoreType.DMA,
        pltpu.SemaphoreType.DMA,
    ]
    vmem = pl.BlockSpec(memory_space=pltpu.VMEM)
    small = jax.ShapeDtypeStruct((LEVELS,), f32)
    results = (*levels, small, small)
    found = pl.pallas_call(
        functools.partial(kernel, row_devices, col_devices),
        out_shape=tuple(pltpu.VMEM(each.shape, each.dtype) for each in results),
        in_specs=[pl.BlockSpec(memory_space=pltpu.HBM)] * 2,
        out_specs=(vmem,) * len(results),
        scratch_shapes=scratch,
        compiler_params=pltpu.CompilerParams(
            collective_id=0, has_side_effects=True, vmem_limit_bytes=56 * 1024 * 1024
        ),
        name="coarsen_levels",
    )(surface_field, land_words.T)

    return pl.pallas_call(
        hand_over,
        out_shape=results,
        in_specs=[vmem] * len(results),
        out_specs=(pl.BlockSpec(memory_space=pl.ANY),) * len(results),
        scratch_shapes=[pltpu.SemaphoreType.DMA((len(results),))],
        compiler_params=pltpu.CompilerParams(vmem_limit_bytes=8 * 1024 * 1024),
        name="hand_over",
    )(*found)


def hand_over(*refs):
    count = LEVELS + 2
    sources, targets, sems = refs[:count], refs[count : 2 * count], refs[2 * count]
    copies = [
        pltpu.make_async_copy(sources[at], targets[at], sems.at[at]) for at in range(count)
    ]
    for copy in copies:
        copy.start()
    for copy in copies:
        copy.wait()


def solution(mesh):
    return jax.shard_map(
        functools.partial(per_device, mesh.shape["rows"], mesh.shape["cols"]),
        mesh=mesh,
        in_specs=(P("rows", "cols"), P("rows", "cols")),
        out_specs=(P("rows", "cols"),) * LEVELS + (P(), P()),
        check_vma=False,
    )
```

```python
import functools
import math

import jax
import jax.numpy as jnp
from jax import lax
from jax.experimental import pallas as pl
from jax.experimental.pallas import tpu as pltpu
from jax.sharding import PartitionSpec as P

stencil_weights = (0.125, 0.375, 0.375, 0.125)
floor_value = 0.05
mean_eps = 1e-06
LEVELS = 4
LANES = 128
HALO = 16
EDGE = 16
CHUNK = 80
MESH = pl.DeviceIdType.MESH
f32 = jnp.float32
bf16 = jnp.bfloat16


def kernel(
    row_devices,
    col_devices,
    field,
    land_words,
    level_one,
    level_two,
    level_three,
    level_four,
    means_ref,
    maxima_ref,
    fine,
    land,
    words,
    cosines,
    cos_rows,
    send_left,
    send_right,
    side,
    side_words,
    p0,
    c0,
    p1,
    c1,
    p2,
    c2,
    p3,
    c3,
    split0,
    split1,
    split2,
    split3,
    partial0,
    partial1,
    partial2,
    partial3,
    stat_own,
    stat_all,
    load_sem,
    land_sem,
    halo_send,
    halo_recv,
    stat_send,
    stat_recv,
    column_sem,
):
    rows, cols = field.shape
    tiles = cols // LANES
    count_words = land.shape[0]
    row_at = lax.axis_index("rows")
    col_at = lax.axis_index("cols")
    total_rows = rows * row_devices
    has_above = row_at > 0
    has_below = row_at < row_devices - 1

    def device(down, right):
        return (
            lax.rem(row_at + down + row_devices, row_devices),
            lax.rem(col_at + right + col_devices, col_devices),
        )

    others = [
        (down, right)
        for down in range(row_devices)
        for right in range(col_devices)
        if (down, right) != (0, 0)
    ]

    near = [
        (down, right)
        for down, right in others
        if down == 0
        or right == 0
        or (down in (1, row_devices - 1) and right in (1, col_devices - 1))
    ]
    land_load = pltpu.make_async_copy(land_words, land, land_sem)

    def load(tile):
        start = tile * LANES
        return pltpu.make_async_copy(
            field.at[:, pl.ds(start, LANES)],
            fine.at[tile, pl.ds(HALO, rows), :],
            load_sem.at[0 if tile == 0 else 2 if tile < tiles - 1 else 1],
        )

    def settle(ref, sem):
        pltpu.make_async_copy(ref, ref, sem).wait()

    load(0).start()
    load(tiles - 1).start()
    land_load.start()

    barrier = pltpu.get_barrier_semaphore()
    for down, right in near:
        pl.semaphore_signal(barrier, inc=1, device_id=device(down, right), device_id_type=MESH)

    for tile in range(1, tiles - 1):
        load(tile).start()

    def clear(row_start, lane_start):
        fine[:, row_start : row_start + HALO, :] = jnp.zeros((tiles, HALO, LANES), f32)
        words[row_start : row_start + HALO, :] = jnp.zeros((HALO, LANES), jnp.int32)
        here = slice(lane_start, lane_start + LANES)
        side[0:HALO, here] = jnp.zeros((HALO, LANES), f32)
        side[LANES - HALO :, here] = jnp.zeros((HALO, LANES), f32)
        side_words[:, here] = jnp.zeros((8, LANES), jnp.int32)

    @pl.when(jnp.logical_not(has_above))
    def _():
        clear(0, 0)

    @pl.when(jnp.logical_not(has_below))
    def _():
        clear(HALO + rows, LANES + rows)

    load(0).wait()
    load(tiles - 1).wait()
    land_load.wait()
    own_rows = pl.ds(HALO, rows)
    lanes = lax.broadcasted_iota(jnp.int32, (rows, LANES), 1)
    outer = jnp.where(lanes < LANES // 2, fine[0, own_rows, :], fine[tiles - 1, own_rows, :])
    outer = jnp.transpose(outer)
    send_left[...] = outer[0:HALO, :]
    send_right[...] = outer[LANES - HALO :, :]

    pl.semaphore_wait(barrier, len(near))

    first_words = land.at[0:1, :]
    last_words = land.at[count_words - 1 : count_words, :]
    own_lanes = pl.ds(LANES, rows)
    top_lanes = pl.ds(0, LANES)
    bottom_lanes = pl.ds(LANES + rows, LANES)
    ahead = pl.ds(0, LANES)
    behind = pl.ds(rows - LANES, LANES)
    right_side = side.at[0:HALO, :]
    left_side = side.at[LANES - HALO :, :]
    right_words = side_words.at[0:1, :]
    left_words = side_words.at[1:2, :]
    across_plan = (
        (send_left, right_side.at[:, own_lanes], (0, -1)),
        (send_right, left_side.at[:, own_lanes], (0, 1)),
        (first_words, right_words.at[:, own_lanes], (0, -1)),
        (last_words, left_words.at[:, own_lanes], (0, 1)),
    )
    down_across_plan = (
        (send_left.at[:, behind], right_side.at[:, top_lanes], (1, -1)),
        (send_right.at[:, behind], left_side.at[:, top_lanes], (1, 1)),
    )
    down_words_plan = (
        (first_words.at[:, behind], right_words.at[:, top_lanes], (1, -1)),
        (last_words.at[:, behind], left_words.at[:, top_lanes], (1, 1)),
    )
    up_across_plan = (
        (send_left.at[:, ahead], right_side.at[:, bottom_lanes], (-1, -1)),
        (send_right.at[:, ahead], left_side.at[:, bottom_lanes], (-1, 1)),
    )
    up_words_plan = (
        (first_words.at[:, ahead], right_words.at[:, bottom_lanes], (-1, -1)),
        (last_words.at[:, ahead], left_words.at[:, bottom_lanes], (-1, 1)),
    )
    down_plan = (
        (fine.at[:, rows : rows + HALO, :], fine.at[:, 0:HALO, :], (1, 0)),
        (words.at[rows : rows + HALO, :], words.at[0:HALO, :], (1, 0)),
    )
    up_plan = (
        (fine.at[:, HALO : 2 * HALO, :], fine.at[:, HALO + rows :, :], (-1, 0)),
        (words.at[HALO : 2 * HALO, :], words.at[HALO + rows :, :], (-1, 0)),
    )
    plans = (
        across_plan,
        down_across_plan,
        up_across_plan,
        down_words_plan,
        up_words_plan,
        down_plan,
        up_plan,
    )
    downs, ups = (1, 3, 5), (2, 4, 6)

    def settle_halo(which, sem):
        moved = sum(math.prod(source.shape) for source, _, _ in plans[which])
        if moved % (8 * LANES):
            settle(side_words.at[0:1, 0:moved], sem.at[which])
        else:
            settle(fine.at[0, 0 : moved // LANES, :], sem.at[which])

    def copies(which, taken):
        return [
            pltpu.make_async_remote_copy(
                src_ref=source,
                dst_ref=target,
                send_sem=halo_send.at[which],
                recv_sem=halo_recv.at[which],
                device_id=device(down, right),
                device_id_type=MESH,
            )
            for source, target, (down, right) in plans[which][taken]
        ]

    def send(which, taken=slice(None)):
        for copy in copies(which, taken):
            copy.start()

    def send_side(side_at):
        taken = slice(side_at, None, 2)
        send(0, taken)

        @pl.when(has_below)
        def _():
            send(1, taken)
            send(3, taken)

        @pl.when(has_above)
        def _():
            send(2, taken)
            send(4, taken)

    at_end = col_at == col_devices - 1
    send_side(0)

    @pl.when(at_end)
    def _():
        send_side(1)

    @pl.when(jnp.logical_not(at_end))
    def _():
        send_side(1)

    for right in range(1, col_devices):
        pl.semaphore_signal(
            column_sem, inc=1, device_id=device(0, right), device_id_type=MESH
        )

    settle(fine.at[1 : tiles - 1, HALO : HALO + rows, :], load_sem.at[2])
    upright = land[...]
    if count_words < LANES:
        filler = jnp.zeros((LANES - count_words, rows), jnp.int32)
        upright = jnp.concatenate([upright, filler], axis=0)
    words[HALO : HALO + rows, :] = jnp.transpose(upright)

    @pl.when(has_below)
    def _():
        send(5)

    @pl.when(has_above)
    def _():
        send(6)

    blocks = rows // LANES + 2
    packed = cos_rows.shape
    row_index = (
        row_at * rows
        - LANES
        + lax.broadcasted_iota(jnp.int32, packed, 0) * LANES
        + lax.broadcasted_iota(jnp.int32, packed, 1)
    )
    latitude = ((row_index.astype(f32) + 0.5) / total_rows - 0.5) * math.pi
    on_globe = jnp.logical_and(row_index >= 0, row_index < total_rows)
    cos_rows[...] = jnp.where(on_globe, jnp.cos(latitude), 0.0)

    def placed(block):
        if block == 0:
            return slice(LANES - HALO, LANES), 0
        if block == blocks - 1:
            return slice(0, HALO), HALO + rows
        return slice(0, LANES), HALO + (block - 1) * LANES

    for block in range(blocks):
        taken, at = placed(block)
        spread = jnp.broadcast_to(cos_rows[block : block + 1, :], (LANES, LANES))
        cosines[at : at + taken.stop - taken.start, :] = jnp.transpose(spread)[taken, :]

    for product, cover, width in ((p0, c0, 8), (p1, c1, 16), (p2, c2, 16), (p3, c3, 16)):
        for ref in (product, cover):
            shape = (ref.shape[0], width, LANES)
            ref[:, 0:width, :] = jnp.zeros(shape, f32)
            ref[:, ref.shape[1] - width :, :] = jnp.zeros(shape, f32)

    def decode(tile, start, count):
        lanes = lax.broadcasted_iota(jnp.int32, (count, LANES), 1)
        place = tile * (LANES // 32) + lax.shift_right_logical(lanes, 5)
        word = jnp.take_along_axis(
            words[pl.ds(start, count), :], place, axis=1, mode="promise_in_bounds"
        )
        bit = lax.shift_left(jnp.ones_like(lanes), jnp.bitwise_and(lanes, 31))
        cover = jnp.where(
            jnp.bitwise_and(word, bit) != 0, cosines[pl.ds(start, count), :], 0.0
        )
        c0[tile, pl.ds(8 + start, count), :] = cover
        p0[tile, pl.ds(8 + start, count), :] = cover * fine[tile, pl.ds(start, count), :]

    sources = ((p0, c0), (p1, c1), (p2, c2), (p3, c3))
    splits = (split0, split1, split2, split3)
    partials = (partial0, partial1, partial2, partial3)
    outputs = (level_one, level_two, level_three, level_four)

    def filtered(level, tile, first, count):
        halves = []
        for ref in sources[level]:
            taps = [ref[tile, pl.ds(7 + a + 2 * first, count, stride=2), :] for a in range(4)]
            down = (taps[0] + taps[3]) + 3.0 * (taps[1] + taps[2])
            high = down.astype(bf16)
            halves += [high, (down - high.astype(f32)).astype(bf16)]
        return halves

    def downward(level, tile, first, count, target):
        for place, half in enumerate(filtered(level, tile, first, count)):
            target[place * count : (place + 1) * count, tile * LANES : (tile + 1) * LANES] = half

    def table(tap, keep=True):
        weight = jnp.where(
            jnp.logical_or(tap == 0, tap == 3),
            stencil_weights[0] / 8.0,
            jnp.where(jnp.logical_or(tap == 1, tap == 2), stencil_weights[1] / 8.0, 0.0),
        )
        return jnp.where(keep, weight, 0.0).astype(bf16)

    band_row = lax.broadcasted_iota(jnp.int32, (4 * LANES, LANES), 0)
    band_col = lax.broadcasted_iota(jnp.int32, (4 * LANES, LANES), 1)
    band = table(band_row - (LANES - 1) - 2 * band_col)

    half = LANES // 2

    def column(at):
        middle = jnp.where(at == half, 0, -1)
        away = jnp.where(at > half, at - LANES, at)
        return jnp.where(jnp.logical_or(at == half, at == half - 1), middle, away)

    lane_in = lax.broadcasted_iota(jnp.int32, (LANES, LANES), 0)
    fine_in = jnp.where(
        lane_in < half, lane_in % HALO, LANES - 1 - (LANES - 1 - lane_in) % HALO
    )
    lane_out = lax.broadcasted_iota(jnp.int32, (LANES, LANES), 1)
    leftward = lane_out >= half
    from_side = table(
        column(lane_in) - 2 * column(lane_out) + 1, (lane_in >= half) == leftward
    )
    from_side_fine = table(
        column(fine_in) - 2 * column(lane_out) + 1, (lane_in >= half) == leftward
    )
    from_first = table(lane_in - 2 * column(lane_out) + 1, leftward)
    from_last = table(lane_in - LANES - 2 * column(lane_out) + 1, jnp.logical_not(leftward))

    def across(count, parts):
        result = None
        for operand, weights in parts:
            part = jnp.dot(operand, weights, preferred_element_type=f32)
            result = part if result is None else result + part
        num = result[0:count] + result[count : 2 * count]
        den = result[2 * count : 3 * count] + result[3 * count :]
        return num, den

    def window(level, start, stop):
        return splits[level][:, start * LANES : stop * LANES]

    def own_parts(tile, tiles_in):
        start = max(2 * tile - 1, 0)
        stop = min(2 * tile + 3, tiles_in)
        skip = start - (2 * tile - 1)
        return start, stop, band[skip * LANES : (skip + stop - start) * LANES]

    def finish(num, den):
        value = num / jnp.maximum(den, floor_value)
        return value, den, den * value

    def ring(shape, tile, count_tiles):
        lanes = lax.broadcasted_iota(jnp.int32, shape, 1)
        if tile == count_tiles:
            return jnp.logical_or(lanes == half, lanes == half - 1)
        here = None
        if tile == 0:
            here = lanes == 0
        if tile == count_tiles - 1:
            final = lanes == LANES - 1
            here = final if here is None else jnp.logical_or(here, final)
        return here

    def tally(stat, value, cover, product):
        def parts(array):
            return array.reshape(array.shape[0] // 8, 8, LANES)

        weighted, total, largest = stat
        return (
            weighted + jnp.sum(parts(product), axis=0),
            total + jnp.sum(parts(cover), axis=0),
            jnp.maximum(largest, jnp.max(parts(value), axis=0)),
        )

    def masked(level, tile, value, cover, product):
        count_tiles = outputs[level].shape[1] // LANES
        here = ring(value.shape, tile, count_tiles)
        if tile == count_tiles:
            inside = jnp.where(here, value, -jnp.inf)
            return cover, product, (inside, jnp.where(here, cover, 0.0), jnp.where(here, product, 0.0))
        if here is not None:
            value = jnp.where(here, -jnp.inf, value)
            cover = jnp.where(here, 0.0, cover)
            product = jnp.where(here, 0.0, product)
        return cover, product, (value, cover, product)

    zero = jnp.zeros((8, LANES), f32)
    stats = [(zero, zero, jnp.full((8, LANES), -jnp.inf, f32)) for _ in range(LEVELS)]
    above_factor = jnp.where(has_above, 1.0, 0.0).astype(f32)
    below_factor = jnp.where(has_below, 1.0, 0.0).astype(f32)

    def inner_rows(level):
        return outputs[level].shape[0] + 16 - 2 * EDGE

    def inner_tile(level, tile, num, den, first=0):
        inner = num.shape[0]
        value, cover, product = finish(num, den)
        cover, product, counted = masked(level, tile, value, cover, product)
        if level + 1 < LEVELS:
            for ref, array in zip(sources[level + 1], (product, cover)):
                ref[tile, 16 + EDGE + first : 16 + EDGE + first + inner, :] = array
        stats[level] = tally(stats[level], *counted)
        return value

    for level in range(LEVELS):
        inner = inner_rows(level)
        tiles_in = sources[level][0].shape[0] - 1
        tiles_out = outputs[level].shape[1] // LANES

        def feed(tile):
            if level == 0:
                for start in range(0, rows, 64):
                    decode(tile, HALO + start, 64)
            downward(level, tile, EDGE, inner, splits[level])

        fed = 0
        for tile in range(tiles_out):
            while fed < min(2 * tile + 3, tiles_in):
                feed(fed)
                fed += 1
            start, stop, weights = own_parts(tile, tiles_in)
            parts = ((window(level, start, stop), weights),)
            value = inner_tile(level, tile, *across(inner, parts))
            lanes = slice(tile * LANES, (tile + 1) * LANES)
            outputs[level][EDGE - 8 : EDGE - 8 + inner, lanes] = value
        parts = (
            (window(level, 0, 1), from_first),
            (window(level, tiles_in - 1, tiles_in), from_last),
        )
        num, den = across(inner, parts)
        partials[level][0] = num
        partials[level][1] = den

    settle_halo(0, halo_recv)

    @pl.when(has_below)
    def _():
        for which in ups:
            settle_halo(which, halo_recv)

    @pl.when(has_above)
    def _():
        for which in downs:
            settle_halo(which, halo_recv)

    sub = lax.broadcasted_iota(jnp.int32, (HALO, LANES), 0)
    turned_lane = lax.broadcasted_iota(jnp.int32, (LANES, LANES), 1)
    turned_slot = jnp.minimum(turned_lane, LANES - 1 - turned_lane) // HALO
    filler = jnp.zeros((LANES - 8 * HALO, LANES), f32)
    for pair in range(blocks // 2):
        both = (pair, blocks - 1 - pair)
        ends = ([], [])
        for block in both:
            here = slice(block * LANES, (block + 1) * LANES)
            turn = jnp.broadcast_to(cos_rows[block : block + 1, :], (HALO, LANES))
            for index, (at, shift) in enumerate(((0, 0), (LANES - HALO, 32 - HALO))):
                word = jnp.broadcast_to(side_words[index : index + 1, here], (HALO, LANES))
                flag = jnp.bitwise_and(lax.shift_right_logical(word, sub + shift), 1)
                cover = jnp.where(flag != 0, turn, 0.0)
                ends[index].extend((cover, cover * side[at : at + HALO, here]))
        pieces = ends[0] + ([filler] if filler.shape[0] else []) + ends[1][::-1]
        flat = jnp.transpose(jnp.concatenate(pieces, axis=0))
        for index, block in enumerate(both):
            taken, at = placed(block)
            size = taken.stop - taken.start
            for kind, ref in ((0, c0), (1, p0)):
                held = jnp.where(turned_slot == 2 * index + kind, flat, 0.0)
                ref[tiles, 8 + at : 8 + at + size, :] = held[taken, :]

    for tile in range(tiles):
        decode(tile, 0, HALO)
        decode(tile, HALO + rows, HALO)

    ring_values = []
    for level in range(LEVELS):
        inner = inner_rows(level)
        output = outputs[level]
        own = output.shape[0]
        tiles_in = sources[level][0].shape[0] - 1
        tiles_out = output.shape[1] // LANES
        side_weights = from_side_fine if level == 0 else from_side
        strips = []
        for tile in range(tiles_in + 1):
            top = filtered(level, tile, 0, EDGE)
            bottom = filtered(level, tile, EDGE + inner, EDGE)
            pieces = [piece for pair in zip(top, bottom) for piece in pair]
            strips.append(jnp.concatenate(pieces, axis=0))
        inner_values = []
        for first in range(0, inner, CHUNK):
            count = min(CHUNK, inner - first)
            operand = jnp.concatenate(filtered(level, tiles_in, EDGE + first, count), axis=0)
            num, den = across(count, ((operand, side_weights),))
            here = slice(first, first + count)
            num, den = num + partials[level][0, here, :], den + partials[level][1, here, :]
            inner_values.append(inner_tile(level, tiles_out, num, den, first))
        inner_value = jnp.concatenate(inner_values, axis=0)
        for tile in range(tiles_out + 1):
            if tile == tiles_out:
                parts = (
                    (strips[tiles_in - 1], from_last),
                    (strips[tiles_in], side_weights),
                    (strips[0], from_first),
                )
            else:
                start, stop, weights = own_parts(tile, tiles_in)
                parts = ((jnp.concatenate(strips[start:stop], axis=1), weights),)
            value, cover, product = finish(*across(2 * EDGE, parts))
            cover, product, counted = masked(level, tile, value, cover, product)
            if level + 1 < LEVELS:
                for ref, array in zip(sources[level + 1], (product, cover)):
                    ref[tile, 16:24, :] = array[0:8] * above_factor
                    ref[tile, 24 : 16 + EDGE, :] = array[8:EDGE]
                    ref[tile, 16 + EDGE + inner : 24 + own, :] = array[EDGE : 2 * EDGE - 8]
                    ref[tile, 24 + own : 32 + own, :] = array[2 * EDGE - 8 :] * below_factor
            middle = slice(8, 2 * EDGE - 8)
            stats[level] = tally(stats[level], *(array[middle] for array in counted))
            if tile < tiles_out:
                lanes = slice(tile * LANES, (tile + 1) * LANES)
                output[0 : EDGE - 8, lanes] = value[8:EDGE]
                output[own - EDGE + 8 :, lanes] = value[EDGE : 2 * EDGE - 8]
            else:
                ring_values.append((inner_value, value[middle]))

    lane = lax.broadcasted_iota(jnp.int32, (8, LANES), 1)
    row = lax.broadcasted_iota(jnp.int32, (8, LANES), 0)
    mine = zero
    for level, (weighted, total, largest) in enumerate(stats):
        weighted = jnp.sum(weighted, axis=0, keepdims=True)
        total = jnp.sum(total, axis=0, keepdims=True)
        sums = jnp.sum(jnp.where(row == 0, weighted, total), axis=1, keepdims=True)
        largest = jnp.max(largest, axis=0, keepdims=True)
        largest = jnp.max(jnp.broadcast_to(largest, (8, LANES)), axis=1, keepdims=True)
        mine = jnp.where(lane == level, jnp.where(row < 2, sums, largest), mine)
    stat_own[...] = mine
    pl.semaphore_wait(column_sem, col_devices - 1)
    far_first = sorted(enumerate(others), key=lambda other: (other[1][1] == 0, other[1][1]))
    for place, (down, right) in far_first:
        copy = pltpu.make_async_remote_copy(
            src_ref=stat_own.at[0:4],
            dst_ref=stat_all.at[place, 0:4],
            send_sem=stat_send,
            recv_sem=stat_recv,
            device_id=device(down, right),
            device_id_type=MESH,
        )
        copy.start()

    for output, (inner_value, edge_value) in zip(outputs, ring_values):
        own, width = output.shape
        tiles_out = width // LANES
        for start, array in (
            (0, edge_value[0:8]),
            (8, inner_value),
            (own - 8, edge_value[8:16]),
        ):
            turned = pltpu.roll(array, half, axis=1)
            here = slice(start, start + array.shape[0])
            for tile in sorted({0, tiles_out - 1}):
                lanes = slice(tile * LANES, (tile + 1) * LANES)
                at_ring = ring(array.shape, tile, tiles_out)
                output[here, lanes] = jnp.where(at_ring, turned, output[here, lanes])

    settle_halo(0, halo_send)

    @pl.when(has_below)
    def _():
        for which in downs:
            settle_halo(which, halo_send)

    @pl.when(has_above)
    def _():
        for which in ups:
            settle_halo(which, halo_send)

    arrived = stat_all.at[:, 0:4, :]
    settle(arrived, stat_recv)

    def combine(reduce):
        parts = [stat_own[0:4, :]] + [stat_all[place, 0:4, :] for place in range(len(others))]
        while len(parts) > 1:
            pairs = [reduce(*pair) for pair in zip(parts[0::2], parts[1::2])]
            parts = pairs + parts[2 * len(pairs) :]
        return parts[0]

    summed, largest = combine(jnp.add), combine(jnp.maximum)
    means_ref[...] = jnp.sum(summed[0:1] / (summed[1:2] + mean_eps), axis=0)[0:LEVELS]
    maxima_ref[...] = jnp.sum(largest[2:3], axis=0)[0:LEVELS]
    settle(arrived, stat_send)


def per_device(row_devices, col_devices, surface_field, land_words):
    rows, cols = surface_field.shape
    tiles = cols // LANES
    levels = tuple(
        jax.ShapeDtypeStruct((rows >> level, cols >> level), f32) for level in range(1, LEVELS + 1)
    )
    blocks = rows // LANES + 2
    scratch = [
        pltpu.VMEM((tiles, rows + 2 * HALO, LANES), f32),
        pltpu.VMEM((land_words.shape[1], rows), jnp.int32),
        pltpu.VMEM((rows + 2 * HALO, LANES), jnp.int32),
        pltpu.VMEM((rows + 2 * HALO, LANES), f32),
        pltpu.VMEM((8 * (-(-blocks // 8)), LANES), f32),
        pltpu.VMEM((HALO, rows), f32),
        pltpu.VMEM((HALO, rows), f32),
        pltpu.VMEM((LANES, rows + 2 * LANES), f32),
        pltpu.VMEM((8, rows + 2 * LANES), jnp.int32),
    ]
    for level in range(LEVELS):
        shape = ((cols >> level) // LANES + 1, (rows >> level) + 48, LANES)
        scratch += [pltpu.VMEM(shape, f32)] * 2
    for level in range(LEVELS):
        inner = (rows >> (level + 1)) + 16 - 2 * EDGE
        scratch.append(pltpu.VMEM((4 * inner, cols >> level), bf16))
    for level in range(LEVELS):
        inner = (rows >> (level + 1)) + 16 - 2 * EDGE
        scratch.append(pltpu.VMEM((2, inner, LANES), f32))
    others = row_devices * col_devices - 1
    scratch += [
        pltpu.VMEM((8, LANES), f32),
        pltpu.VMEM((others, 8, LANES), f32),
        pltpu.SemaphoreType.DMA((3,)),
        pltpu.SemaphoreType.DMA,
        pltpu.SemaphoreType.DMA((7,)),
        pltpu.SemaphoreType.DMA((7,)),
        pltpu.SemaphoreType.DMA,
        pltpu.SemaphoreType.DMA,
        pltpu.SemaphoreType.REGULAR,
    ]
    vmem = pl.BlockSpec(memory_space=pltpu.VMEM)
    small = jax.ShapeDtypeStruct((LEVELS,), f32)
    results = (*levels, small, small)
    found = pl.pallas_call(
        functools.partial(kernel, row_devices, col_devices),
        out_shape=tuple(pltpu.VMEM(each.shape, each.dtype) for each in results),
        in_specs=[pl.BlockSpec(memory_space=pltpu.HBM)] * 2,
        out_specs=(vmem,) * len(results),
        scratch_shapes=scratch,
        compiler_params=pltpu.CompilerParams(
            collective_id=0, has_side_effects=True, vmem_limit_bytes=56 * 1024 * 1024
        ),
        name="coarsen_levels",
    )(surface_field, land_words.T)

    return pl.pallas_call(
        hand_over,
        out_shape=results,
        in_specs=[vmem] * len(results),
        out_specs=(pl.BlockSpec(memory_space=pl.ANY),) * len(results),
        scratch_shapes=[pltpu.SemaphoreType.DMA((len(results),))],
        compiler_params=pltpu.CompilerParams(vmem_limit_bytes=8 * 1024 * 1024),
        name="hand_over",
    )(*found)


def hand_over(*refs):
    count = LEVELS + 2
    sources, targets, sems = refs[:count], refs[count : 2 * count], refs[2 * count]
    copies = [
        pltpu.make_async_copy(sources[at], targets[at], sems.at[at]) for at in range(count)
    ]
    for copy in copies:
        copy.start()
    for copy in copies:
        copy.wait()


def solution(mesh):
    return jax.shard_map(
        functools.partial(per_device, mesh.shape["rows"], mesh.shape["cols"]),
        mesh=mesh,
        in_specs=(P("rows", "cols"), P("rows", "cols")),
        out_specs=(P("rows", "cols"),) * LEVELS + (P(), P()),
        check_vma=False,
    )
```

```python
import functools
import math

import jax
import jax.numpy as jnp
from jax import lax
from jax.experimental import pallas as pl
from jax.experimental.pallas import tpu as pltpu
from jax.sharding import PartitionSpec as P

stencil_weights = (0.125, 0.375, 0.375, 0.125)
floor_value = 0.05
mean_eps = 1e-06
LEVELS = 4
LANES = 128
HALO = 16
EDGE = 16
CHUNK = 80
MESH = pl.DeviceIdType.MESH
f32 = jnp.float32
bf16 = jnp.bfloat16


def kernel(
    row_devices,
    col_devices,
    field,
    land_words,
    level_one,
    level_two,
    level_three,
    level_four,
    means_ref,
    maxima_ref,
    fine,
    land,
    words,
    cosines,
    cos_rows,
    send_left,
    send_right,
    side,
    side_words,
    p0,
    c0,
    p1,
    c1,
    p2,
    c2,
    p3,
    c3,
    split0,
    split1,
    split2,
    split3,
    partial0,
    partial1,
    partial2,
    partial3,
    stat_own,
    stat_all,
    load_sem,
    land_sem,
    halo_send,
    halo_recv,
    stat_send,
    stat_recv,
    column_sem,
    from_above_sem,
    from_below_sem,
):
    rows, cols = field.shape
    tiles = cols // LANES
    count_words = land.shape[0]
    row_at = lax.axis_index("rows")
    col_at = lax.axis_index("cols")
    total_rows = rows * row_devices
    has_above = row_at > 0
    has_below = row_at < row_devices - 1

    def device(down, right):
        return (
            lax.rem(row_at + down + row_devices, row_devices),
            lax.rem(col_at + right + col_devices, col_devices),
        )

    others = [
        (down, right)
        for down in range(row_devices)
        for right in range(col_devices)
        if (down, right) != (0, 0)
    ]

    near = [(down, right) for down, right in others if down == 0 or right == 0]

    land_load = pltpu.make_async_copy(land_words, land, land_sem)

    def load(tile):
        start = tile * LANES
        return pltpu.make_async_copy(
            field.at[:, pl.ds(start, LANES)],
            fine.at[tile, pl.ds(HALO, rows), :],
            load_sem.at[0 if tile == 0 else 2 if tile < tiles - 1 else 1],
        )

    def settle(ref, sem):
        pltpu.make_async_copy(ref, ref, sem).wait()

    load(0).start()
    load(tiles - 1).start()
    land_load.start()

    barrier = pltpu.get_barrier_semaphore()
    for down, right in near:
        pl.semaphore_signal(barrier, inc=1, device_id=device(down, right), device_id_type=MESH)

    for tile in range(1, tiles - 1):
        load(tile).start()

    def clear(row_start, lane_start):
        fine[:, row_start : row_start + HALO, :] = jnp.zeros((tiles, HALO, LANES), f32)
        words[row_start : row_start + HALO, :] = jnp.zeros((HALO, LANES), jnp.int32)
        here = slice(lane_start, lane_start + LANES)
        side[0:HALO, here] = jnp.zeros((HALO, LANES), f32)
        side[LANES - HALO :, here] = jnp.zeros((HALO, LANES), f32)
        side_words[:, here] = jnp.zeros((8, LANES), jnp.int32)

    @pl.when(jnp.logical_not(has_above))
    def _():
        clear(0, 0)

    @pl.when(jnp.logical_not(has_below))
    def _():
        clear(HALO + rows, LANES + rows)

    load(0).wait()
    load(tiles - 1).wait()
    land_load.wait()
    own_rows = pl.ds(HALO, rows)
    lanes = lax.broadcasted_iota(jnp.int32, (rows, LANES), 1)
    outer = jnp.where(lanes < LANES // 2, fine[0, own_rows, :], fine[tiles - 1, own_rows, :])
    outer = jnp.transpose(outer)
    send_left[...] = outer[0:HALO, :]
    send_right[...] = outer[LANES - HALO :, :]

    upright = land[...]
    if count_words < LANES:
        filler = jnp.zeros((LANES - count_words, rows), jnp.int32)
        upright = jnp.concatenate([upright, filler], axis=0)
    words[HALO : HALO + rows, :] = jnp.transpose(upright)

    pl.semaphore_wait(barrier, len(near))

    first_words = land.at[0:1, :]
    last_words = land.at[count_words - 1 : count_words, :]
    own_lanes = pl.ds(LANES, rows)
    top_lanes = pl.ds(0, LANES)
    bottom_lanes = pl.ds(LANES + rows, LANES)
    ahead = pl.ds(0, LANES)
    behind = pl.ds(rows - LANES, LANES)
    right_side = side.at[0:HALO, :]
    left_side = side.at[LANES - HALO :, :]
    right_words = side_words.at[0:1, :]
    left_words = side_words.at[1:2, :]
    across_plan = (
        (send_left, right_side.at[:, own_lanes], (0, -1)),
        (send_right, left_side.at[:, own_lanes], (0, 1)),
        (first_words, right_words.at[:, own_lanes], (0, -1)),
        (last_words, left_words.at[:, own_lanes], (0, 1)),
    )
    down_across_plan = (
        (send_left.at[:, behind], right_side.at[:, top_lanes], (1, -1)),
        (send_right.at[:, behind], left_side.at[:, top_lanes], (1, 1)),
    )
    down_words_plan = (
        (first_words.at[:, behind], right_words.at[:, top_lanes], (1, -1)),
        (last_words.at[:, behind], left_words.at[:, top_lanes], (1, 1)),
    )
    up_across_plan = (
        (send_left.at[:, ahead], right_side.at[:, bottom_lanes], (-1, -1)),
        (send_right.at[:, ahead], left_side.at[:, bottom_lanes], (-1, 1)),
    )
    up_words_plan = (
        (first_words.at[:, ahead], right_words.at[:, bottom_lanes], (-1, -1)),
        (last_words.at[:, ahead], left_words.at[:, bottom_lanes], (-1, 1)),
    )
    down_plan = (
        (fine.at[:, rows : rows + HALO, :], fine.at[:, 0:HALO, :], (1, 0)),
        (words.at[rows : rows + HALO, :], words.at[0:HALO, :], (1, 0)),
    )
    up_plan = (
        (fine.at[:, HALO : 2 * HALO, :], fine.at[:, HALO + rows :, :], (-1, 0)),
        (words.at[HALO : 2 * HALO, :], words.at[HALO + rows :, :], (-1, 0)),
    )
    plans = (
        across_plan,
        down_across_plan,
        up_across_plan,
        down_words_plan,
        up_words_plan,
        down_plan,
        up_plan,
    )
    downs, ups = (1, 3, 5), (2, 4, 6)

    def settle_halo(which, sem):
        moved = sum(math.prod(source.shape) for source, _, _ in plans[which])
        if moved % (8 * LANES):
            settle(side_words.at[0:1, 0:moved], sem.at[which])
        else:
            settle(fine.at[0, 0 : moved // LANES, :], sem.at[which])

    def copies(which, taken):
        return [
            pltpu.make_async_remote_copy(
                src_ref=source,
                dst_ref=target,
                send_sem=halo_send.at[which],
                recv_sem=halo_recv.at[which],
                device_id=device(down, right),
                device_id_type=MESH,
            )
            for source, target, (down, right) in plans[which][taken]
        ]

    def send(which, taken=slice(None)):
        for copy in copies(which, taken):
            copy.start()

    send(0, slice(0, None, 2))
    send(0, slice(1, None, 2))

    @pl.when(has_below)
    def _():
        pl.semaphore_signal(
            from_above_sem, inc=1, device_id=device(1, 0), device_id_type=MESH
        )

    @pl.when(has_above)
    def _():
        pl.semaphore_signal(
            from_below_sem, inc=1, device_id=device(-1, 0), device_id_type=MESH
        )

    for right in range(1, col_devices):
        pl.semaphore_signal(
            column_sem, inc=1, device_id=device(0, right), device_id_type=MESH
        )

    settle(fine.at[1 : tiles - 1, HALO : HALO + rows, :], load_sem.at[2])
    @pl.when(has_below)
    def _():
        send(5)

    @pl.when(has_above)
    def _():
        send(6)

    @pl.when(has_below)
    def _():
        pl.semaphore_wait(from_below_sem, 1)

    @pl.when(has_above)
    def _():
        pl.semaphore_wait(from_above_sem, 1)

    for side_at in range(2):
        taken = slice(side_at, None, 2)

        @pl.when(has_below)
        def _():
            send(1, taken)
            send(3, taken)

        @pl.when(has_above)
        def _():
            send(2, taken)
            send(4, taken)

    blocks = rows // LANES + 2
    packed = cos_rows.shape
    row_index = (
        row_at * rows
        - LANES
        + lax.broadcasted_iota(jnp.int32, packed, 0) * LANES
        + lax.broadcasted_iota(jnp.int32, packed, 1)
    )
    latitude = ((row_index.astype(f32) + 0.5) / total_rows - 0.5) * math.pi
    on_globe = jnp.logical_and(row_index >= 0, row_index < total_rows)
    cos_rows[...] = jnp.where(on_globe, jnp.cos(latitude), 0.0)

    def placed(block):
        if block == 0:
            return slice(LANES - HALO, LANES), 0
        if block == blocks - 1:
            return slice(0, HALO), HALO + rows
        return slice(0, LANES), HALO + (block - 1) * LANES

    for block in range(blocks):
        taken, at = placed(block)
        spread = jnp.broadcast_to(cos_rows[block : block + 1, :], (LANES, LANES))
        cosines[at : at + taken.stop - taken.start, :] = jnp.transpose(spread)[taken, :]

    for product, cover, width in ((p0, c0, 8), (p1, c1, 16), (p2, c2, 16), (p3, c3, 16)):
        for ref in (product, cover):
            shape = (ref.shape[0], width, LANES)
            ref[:, 0:width, :] = jnp.zeros(shape, f32)
            ref[:, ref.shape[1] - width :, :] = jnp.zeros(shape, f32)

    def decode(tile, start, count):
        lanes = lax.broadcasted_iota(jnp.int32, (count, LANES), 1)
        place = tile * (LANES // 32) + lax.shift_right_logical(lanes, 5)
        word = jnp.take_along_axis(
            words[pl.ds(start, count), :], place, axis=1, mode="promise_in_bounds"
        )
        bit = lax.shift_left(jnp.ones_like(lanes), jnp.bitwise_and(lanes, 31))
        cover = jnp.where(
            jnp.bitwise_and(word, bit) != 0, cosines[pl.ds(start, count), :], 0.0
        )
        c0[tile, pl.ds(8 + start, count), :] = cover
        p0[tile, pl.ds(8 + start, count), :] = cover * fine[tile, pl.ds(start, count), :]

    sources = ((p0, c0), (p1, c1), (p2, c2), (p3, c3))
    splits = (split0, split1, split2, split3)
    partials = (partial0, partial1, partial2, partial3)
    outputs = (level_one, level_two, level_three, level_four)

    def filtered(level, tile, first, count):
        halves = []
        for ref in sources[level]:
            taps = [ref[tile, pl.ds(7 + a + 2 * first, count, stride=2), :] for a in range(4)]
            down = (taps[0] + taps[3]) + 3.0 * (taps[1] + taps[2])
            high = down.astype(bf16)
            halves += [high, (down - high.astype(f32)).astype(bf16)]
        return halves

    def downward(level, tile, first, count, target):
        for place, half in enumerate(filtered(level, tile, first, count)):
            target[place * count : (place + 1) * count, tile * LANES : (tile + 1) * LANES] = half

    def table(tap, keep=True):
        weight = jnp.where(
            jnp.logical_or(tap == 0, tap == 3),
            stencil_weights[0] / 8.0,
            jnp.where(jnp.logical_or(tap == 1, tap == 2), stencil_weights[1] / 8.0, 0.0),
        )
        return jnp.where(keep, weight, 0.0).astype(bf16)

    band_row = lax.broadcasted_iota(jnp.int32, (4 * LANES, LANES), 0)
    band_col = lax.broadcasted_iota(jnp.int32, (4 * LANES, LANES), 1)
    band = table(band_row - (LANES - 1) - 2 * band_col)

    half = LANES // 2

    def column(at):
        middle = jnp.where(at == half, 0, -1)
        away = jnp.where(at > half, at - LANES, at)
        return jnp.where(jnp.logical_or(at == half, at == half - 1), middle, away)

    lane_in = lax.broadcasted_iota(jnp.int32, (LANES, LANES), 0)
    fine_in = jnp.where(
        lane_in < half, lane_in % HALO, LANES - 1 - (LANES - 1 - lane_in) % HALO
    )
    lane_out = lax.broadcasted_iota(jnp.int32, (LANES, LANES), 1)
    leftward = lane_out >= half
    from_side = table(
        column(lane_in) - 2 * column(lane_out) + 1, (lane_in >= half) == leftward
    )
    from_side_fine = table(
        column(fine_in) - 2 * column(lane_out) + 1, (lane_in >= half) == leftward
    )
    from_first = table(lane_in - 2 * column(lane_out) + 1, leftward)
    from_last = table(lane_in - LANES - 2 * column(lane_out) + 1, jnp.logical_not(leftward))

    def across(count, parts):
        result = None
        for operand, weights in parts:
            part = jnp.dot(operand, weights, preferred_element_type=f32)
            result = part if result is None else result + part
        num = result[0:count] + result[count : 2 * count]
        den = result[2 * count : 3 * count] + result[3 * count :]
        return num, den

    def window(level, start, stop):
        return splits[level][:, start * LANES : stop * LANES]

    def own_parts(tile, tiles_in):
        start = max(2 * tile - 1, 0)
        stop = min(2 * tile + 3, tiles_in)
        skip = start - (2 * tile - 1)
        return start, stop, band[skip * LANES : (skip + stop - start) * LANES]

    def finish(num, den):
        value = num / jnp.maximum(den, floor_value)
        return value, den, den * value

    def ring(shape, tile, count_tiles):
        lanes = lax.broadcasted_iota(jnp.int32, shape, 1)
        if tile == count_tiles:
            return jnp.logical_or(lanes == half, lanes == half - 1)
        here = None
        if tile == 0:
            here = lanes == 0
        if tile == count_tiles - 1:
            final = lanes == LANES - 1
            here = final if here is None else jnp.logical_or(here, final)
        return here

    def tally(stat, value, cover, product):
        def parts(array):
            return array.reshape(array.shape[0] // 8, 8, LANES)

        weighted, total, largest = stat
        return (
            weighted + jnp.sum(parts(product), axis=0),
            total + jnp.sum(parts(cover), axis=0),
            jnp.maximum(largest, jnp.max(parts(value), axis=0)),
        )

    def masked(level, tile, value, cover, product):
        count_tiles = outputs[level].shape[1] // LANES
        here = ring(value.shape, tile, count_tiles)
        if tile == count_tiles:
            inside = jnp.where(here, value, -jnp.inf)
            return cover, product, (inside, jnp.where(here, cover, 0.0), jnp.where(here, product, 0.0))
        if here is not None:
            value = jnp.where(here, -jnp.inf, value)
            cover = jnp.where(here, 0.0, cover)
            product = jnp.where(here, 0.0, product)
        return cover, product, (value, cover, product)

    zero = jnp.zeros((8, LANES), f32)
    stats = [(zero, zero, jnp.full((8, LANES), -jnp.inf, f32)) for _ in range(LEVELS)]
    above_factor = jnp.where(has_above, 1.0, 0.0).astype(f32)
    below_factor = jnp.where(has_below, 1.0, 0.0).astype(f32)

    def inner_rows(level):
        return outputs[level].shape[0] + 16 - 2 * EDGE

    def inner_tile(level, tile, num, den, first=0):
        inner = num.shape[0]
        value, cover, product = finish(num, den)
        cover, product, counted = masked(level, tile, value, cover, product)
        if level + 1 < LEVELS:
            for ref, array in zip(sources[level + 1], (product, cover)):
                ref[tile, 16 + EDGE + first : 16 + EDGE + first + inner, :] = array
        stats[level] = tally(stats[level], *counted)
        return value

    for level in range(LEVELS):
        inner = inner_rows(level)
        tiles_in = sources[level][0].shape[0] - 1
        tiles_out = outputs[level].shape[1] // LANES

        def feed(tile):
            if level == 0:
                for start in range(0, rows, 64):
                    decode(tile, HALO + start, 64)
            downward(level, tile, EDGE, inner, splits[level])

        fed = 0
        for tile in range(tiles_out):
            while fed < min(2 * tile + 3, tiles_in):
                feed(fed)
                fed += 1
            start, stop, weights = own_parts(tile, tiles_in)
            parts = ((window(level, start, stop), weights),)
            value = inner_tile(level, tile, *across(inner, parts))
            lanes = slice(tile * LANES, (tile + 1) * LANES)
            outputs[level][EDGE - 8 : EDGE - 8 + inner, lanes] = value
        parts = (
            (window(level, 0, 1), from_first),
            (window(level, tiles_in - 1, tiles_in), from_last),
        )
        num, den = across(inner, parts)
        partials[level][0] = num
        partials[level][1] = den

    @pl.when(has_below)
    def _():
        settle_halo(6, halo_recv)

    @pl.when(has_above)
    def _():
        settle_halo(5, halo_recv)

    settle_halo(0, halo_recv)

    @pl.when(has_below)
    def _():
        settle_halo(2, halo_recv)
        settle_halo(4, halo_recv)

    @pl.when(has_above)
    def _():
        settle_halo(1, halo_recv)
        settle_halo(3, halo_recv)

    sub = lax.broadcasted_iota(jnp.int32, (HALO, LANES), 0)
    turned_lane = lax.broadcasted_iota(jnp.int32, (LANES, LANES), 1)
    turned_slot = jnp.minimum(turned_lane, LANES - 1 - turned_lane) // HALO
    filler = jnp.zeros((LANES - 8 * HALO, LANES), f32)
    for pair in range(blocks // 2):
        both = (pair, blocks - 1 - pair)
        ends = ([], [])
        for block in both:
            here = slice(block * LANES, (block + 1) * LANES)
            turn = jnp.broadcast_to(cos_rows[block : block + 1, :], (HALO, LANES))
            for index, (at, shift) in enumerate(((0, 0), (LANES - HALO, 32 - HALO))):
                word = jnp.broadcast_to(side_words[index : index + 1, here], (HALO, LANES))
                flag = jnp.bitwise_and(lax.shift_right_logical(word, sub + shift), 1)
                cover = jnp.where(flag != 0, turn, 0.0)
                ends[index].extend((cover, cover * side[at : at + HALO, here]))
        pieces = ends[0] + ([filler] if filler.shape[0] else []) + ends[1][::-1]
        flat = jnp.transpose(jnp.concatenate(pieces, axis=0))
        for index, block in enumerate(both):
            taken, at = placed(block)
            size = taken.stop - taken.start
            for kind, ref in ((0, c0), (1, p0)):
                held = jnp.where(turned_slot == 2 * index + kind, flat, 0.0)
                ref[tiles, 8 + at : 8 + at + size, :] = held[taken, :]

    for tile in range(tiles):
        decode(tile, 0, HALO)
        decode(tile, HALO + rows, HALO)

    def keep_strip(level, tile, cover, product):
        inner = inner_rows(level)
        own = outputs[level].shape[0]
        if level + 1 < LEVELS:
            for ref, array in zip(sources[level + 1], (product, cover)):
                ref[tile, 16:24, :] = array[0:8] * above_factor
                ref[tile, 24 : 16 + EDGE, :] = array[8:EDGE]
                ref[tile, 16 + EDGE + inner : 24 + own, :] = array[EDGE : 2 * EDGE - 8]
                ref[tile, 24 + own : 32 + own, :] = array[2 * EDGE - 8 :] * below_factor

    def strip(level, tile):
        top = filtered(level, tile, 0, EDGE)
        bottom = filtered(level, tile, EDGE + inner_rows(level), EDGE)
        return [piece for pair in zip(top, bottom) for piece in pair]

    middle = slice(8, 2 * EDGE - 8)
    def across_side(level, halves):
        weights = from_side_fine if level == 0 else from_side
        weights = jnp.concatenate([weights, weights], axis=0)
        high = jnp.concatenate(halves[0 : len(halves) // 4] + halves[len(halves) // 2 : -(len(halves) // 4)], axis=0)
        low = jnp.concatenate(halves[len(halves) // 4 : len(halves) // 2] + halves[-(len(halves) // 4) :], axis=0)
        count = high.shape[0] // 2
        result = jnp.dot(
            jnp.concatenate([high, low], axis=1), weights, preferred_element_type=f32
        )
        return result[0:count], result[count:]

    ring_values = []
    for level in range(LEVELS):
        output = outputs[level]
        own = output.shape[0]
        tiles_in = sources[level][0].shape[0] - 1
        tiles_out = output.shape[1] // LANES
        strips = [jnp.concatenate(strip(level, tile), axis=0) for tile in range(tiles_in)]
        for tile in range(tiles_out):
            start, stop, weights = own_parts(tile, tiles_in)
            parts = ((jnp.concatenate(strips[start:stop], axis=1), weights),)
            value, cover, product = finish(*across(2 * EDGE, parts))
            cover, product, counted = masked(level, tile, value, cover, product)
            keep_strip(level, tile, cover, product)
            stats[level] = tally(stats[level], *(array[middle] for array in counted))
            lanes = slice(tile * LANES, (tile + 1) * LANES)
            output[0 : EDGE - 8, lanes] = value[8:EDGE]
            output[own - EDGE + 8 :, lanes] = value[EDGE : 2 * EDGE - 8]
        parts = ((strips[tiles_in - 1], from_last), (strips[0], from_first))
        edge_partial = across(2 * EDGE, parts)
        inner = inner_rows(level)
        inner_values = []
        for first in range(0, inner, CHUNK):
            count = min(CHUNK, inner - first)
            num, den = across_side(level, filtered(level, tiles_in, EDGE + first, count))
            here = slice(first, first + count)
            num, den = num + partials[level][0, here, :], den + partials[level][1, here, :]
            inner_values.append(inner_tile(level, tiles_out, num, den, first))
        inner_value = jnp.concatenate(inner_values, axis=0)
        num, den = across_side(level, strip(level, tiles_in))
        num, den = num + edge_partial[0], den + edge_partial[1]
        value, cover, product = finish(num, den)
        cover, product, counted = masked(level, tiles_out, value, cover, product)
        keep_strip(level, tiles_out, cover, product)
        stats[level] = tally(stats[level], *(array[middle] for array in counted))
        ring_values.append((inner_value, value[middle]))

    lane = lax.broadcasted_iota(jnp.int32, (8, LANES), 1)
    row = lax.broadcasted_iota(jnp.int32, (8, LANES), 0)
    mine = zero
    for level, (weighted, total, largest) in enumerate(stats):
        weighted = jnp.sum(weighted, axis=0, keepdims=True)
        total = jnp.sum(total, axis=0, keepdims=True)
        sums = jnp.sum(jnp.where(row == 0, weighted, total), axis=1, keepdims=True)
        largest = jnp.max(largest, axis=0, keepdims=True)
        largest = jnp.max(jnp.broadcast_to(largest, (8, LANES)), axis=1, keepdims=True)
        mine = jnp.where(lane == level, jnp.where(row < 2, sums, largest), mine)
    stat_own[...] = mine
    pl.semaphore_wait(column_sem, col_devices - 1)
    far_first = sorted(enumerate(others), key=lambda other: (other[1][1] == 0, other[1][1]))
    for place, (down, right) in far_first:
        copy = pltpu.make_async_remote_copy(
            src_ref=stat_own.at[0:4],
            dst_ref=stat_all.at[place, 0:4],
            send_sem=stat_send,
            recv_sem=stat_recv,
            device_id=device(down, right),
            device_id_type=MESH,
        )
        copy.start()

    for output, (inner_value, edge_value) in zip(outputs, ring_values):
        own, width = output.shape
        tiles_out = width // LANES
        for start, array in (
            (0, edge_value[0:8]),
            (8, inner_value),
            (own - 8, edge_value[8:16]),
        ):
            turned = pltpu.roll(array, half, axis=1)
            here = slice(start, start + array.shape[0])
            for tile in sorted({0, tiles_out - 1}):
                lanes = slice(tile * LANES, (tile + 1) * LANES)
                at_ring = ring(array.shape, tile, tiles_out)
                output[here, lanes] = jnp.where(at_ring, turned, output[here, lanes])

    settle_halo(0, halo_send)

    @pl.when(has_below)
    def _():
        for which in downs:
            settle_halo(which, halo_send)

    @pl.when(has_above)
    def _():
        for which in ups:
            settle_halo(which, halo_send)

    arrived = stat_all.at[:, 0:4, :]
    settle(arrived, stat_recv)

    def combine(reduce):
        parts = [stat_own[0:4, :]] + [stat_all[place, 0:4, :] for place in range(len(others))]
        while len(parts) > 1:
            pairs = [reduce(*pair) for pair in zip(parts[0::2], parts[1::2])]
            parts = pairs + parts[2 * len(pairs) :]
        return parts[0]

    summed, largest = combine(jnp.add), combine(jnp.maximum)
    means_ref[...] = jnp.sum(summed[0:1] / (summed[1:2] + mean_eps), axis=0)[0:LEVELS]
    maxima_ref[...] = jnp.sum(largest[2:3], axis=0)[0:LEVELS]
    settle(arrived, stat_send)


def per_device(row_devices, col_devices, surface_field, land_words):
    rows, cols = surface_field.shape
    tiles = cols // LANES
    levels = tuple(
        jax.ShapeDtypeStruct((rows >> level, cols >> level), f32) for level in range(1, LEVELS + 1)
    )
    blocks = rows // LANES + 2
    scratch = [
        pltpu.VMEM((tiles, rows + 2 * HALO, LANES), f32),
        pltpu.VMEM((land_words.shape[1], rows), jnp.int32),
        pltpu.VMEM((rows + 2 * HALO, LANES), jnp.int32),
        pltpu.VMEM((rows + 2 * HALO, LANES), f32),
        pltpu.VMEM((8 * (-(-blocks // 8)), LANES), f32),
        pltpu.VMEM((HALO, rows), f32),
        pltpu.VMEM((HALO, rows), f32),
        pltpu.VMEM((LANES, rows + 2 * LANES), f32),
        pltpu.VMEM((8, rows + 2 * LANES), jnp.int32),
    ]
    for level in range(LEVELS):
        shape = ((cols >> level) // LANES + 1, (rows >> level) + 48, LANES)
        scratch += [pltpu.VMEM(shape, f32)] * 2
    for level in range(LEVELS):
        inner = (rows >> (level + 1)) + 16 - 2 * EDGE
        scratch.append(pltpu.VMEM((4 * inner, cols >> level), bf16))
    for level in range(LEVELS):
        inner = (rows >> (level + 1)) + 16 - 2 * EDGE
        scratch.append(pltpu.VMEM((2, inner, LANES), f32))
    others = row_devices * col_devices - 1
    scratch += [
        pltpu.VMEM((8, LANES), f32),
        pltpu.VMEM((others, 8, LANES), f32),
        pltpu.SemaphoreType.DMA((3,)),
        pltpu.SemaphoreType.DMA,
        pltpu.SemaphoreType.DMA((7,)),
        pltpu.SemaphoreType.DMA((7,)),
        pltpu.SemaphoreType.DMA,
        pltpu.SemaphoreType.DMA,
        pltpu.SemaphoreType.REGULAR,
        pltpu.SemaphoreType.REGULAR,
        pltpu.SemaphoreType.REGULAR,
    ]
    vmem = pl.BlockSpec(memory_space=pltpu.VMEM)
    small = jax.ShapeDtypeStruct((LEVELS,), f32)
    results = (*levels, small, small)
    found = pl.pallas_call(
        functools.partial(kernel, row_devices, col_devices),
        out_shape=tuple(pltpu.VMEM(each.shape, each.dtype) for each in results),
        in_specs=[pl.BlockSpec(memory_space=pltpu.HBM)] * 2,
        out_specs=(vmem,) * len(results),
        scratch_shapes=scratch,
        compiler_params=pltpu.CompilerParams(
            collective_id=0, has_side_effects=True, vmem_limit_bytes=56 * 1024 * 1024
        ),
        name="coarsen_levels",
    )(surface_field, land_words.T)

    return pl.pallas_call(
        hand_over,
        out_shape=results,
        in_specs=[vmem] * len(results),
        out_specs=(pl.BlockSpec(memory_space=pl.ANY),) * len(results),
        scratch_shapes=[pltpu.SemaphoreType.DMA((len(results),))],
        compiler_params=pltpu.CompilerParams(vmem_limit_bytes=8 * 1024 * 1024),
        name="hand_over",
    )(*found)


def hand_over(*refs):
    count = LEVELS + 2
    sources, targets, sems = refs[:count], refs[count : 2 * count], refs[2 * count]
    copies = [
        pltpu.make_async_copy(sources[at], targets[at], sems.at[at]) for at in range(count)
    ]
    for copy in copies:
        copy.start()
    for copy in copies:
        copy.wait()


def solution(mesh):
    return jax.shard_map(
        functools.partial(per_device, mesh.shape["rows"], mesh.shape["cols"]),
        mesh=mesh,
        in_specs=(P("rows", "cols"), P("rows", "cols")),
        out_specs=(P("rows", "cols"),) * LEVELS + (P(), P()),
        check_vma=False,
    )
```

```python
import functools
import math

import jax
import jax.numpy as jnp
from jax import lax
from jax.experimental import pallas as pl
from jax.experimental.pallas import tpu as pltpu
from jax.sharding import PartitionSpec as P

stencil_weights = (0.125, 0.375, 0.375, 0.125)
floor_value = 0.05
mean_eps = 1e-06
LEVELS = 4
LANES = 128
HALO = 16
EDGE = 16
CHUNK = 80
MESH = pl.DeviceIdType.MESH
f32 = jnp.float32
bf16 = jnp.bfloat16


def kernel(
    row_devices,
    col_devices,
    field,
    land_words,
    level_one,
    level_two,
    level_three,
    level_four,
    means_ref,
    maxima_ref,
    fine,
    land,
    words,
    cosines,
    cos_rows,
    send_left,
    send_right,
    side,
    side_words,
    p0,
    c0,
    p1,
    c1,
    p2,
    c2,
    p3,
    c3,
    partial0,
    partial1,
    partial2,
    partial3,
    stat_own,
    stat_all,
    load_sem,
    land_sem,
    halo_send,
    halo_recv,
    stat_send,
    stat_recv,
    column_sem,
    from_above_sem,
    from_below_sem,
):
    rows, cols = field.shape
    tiles = cols // LANES
    count_words = land.shape[0]
    row_at = lax.axis_index("rows")
    col_at = lax.axis_index("cols")
    total_rows = rows * row_devices
    has_above = row_at > 0
    has_below = row_at < row_devices - 1

    def device(down, right):
        return (
            lax.rem(row_at + down + row_devices, row_devices),
            lax.rem(col_at + right + col_devices, col_devices),
        )

    others = [
        (down, right)
        for down in range(row_devices)
        for right in range(col_devices)
        if (down, right) != (0, 0)
    ]

    near = [(down, right) for down, right in others if down == 0 or right == 0]

    land_load = pltpu.make_async_copy(land_words, land, land_sem)

    def load(tile):
        start = tile * LANES
        return pltpu.make_async_copy(
            field.at[:, pl.ds(start, LANES)],
            fine.at[tile, pl.ds(HALO, rows), :],
            load_sem.at[0 if tile == 0 else 2 if tile < tiles - 1 else 1],
        )

    def settle(ref, sem):
        pltpu.make_async_copy(ref, ref, sem).wait()

    load(0).start()
    load(tiles - 1).start()
    land_load.start()

    barrier = pltpu.get_barrier_semaphore()
    for down, right in near:
        pl.semaphore_signal(barrier, inc=1, device_id=device(down, right), device_id_type=MESH)

    for tile in range(1, tiles - 1):
        load(tile).start()

    def clear(row_start, lane_start):
        fine[:, row_start : row_start + HALO, :] = jnp.zeros((tiles, HALO, LANES), f32)
        words[row_start : row_start + HALO, :] = jnp.zeros((HALO, LANES), jnp.int32)
        here = slice(lane_start, lane_start + LANES)
        side[0:HALO, here] = jnp.zeros((HALO, LANES), f32)
        side[LANES - HALO :, here] = jnp.zeros((HALO, LANES), f32)
        side_words[:, here] = jnp.zeros((8, LANES), jnp.int32)

    @pl.when(jnp.logical_not(has_above))
    def _():
        clear(0, 0)

    @pl.when(jnp.logical_not(has_below))
    def _():
        clear(HALO + rows, LANES + rows)

    load(0).wait()
    load(tiles - 1).wait()
    land_load.wait()
    own_rows = pl.ds(HALO, rows)
    lanes = lax.broadcasted_iota(jnp.int32, (rows, LANES), 1)
    outer = jnp.where(lanes < LANES // 2, fine[0, own_rows, :], fine[tiles - 1, own_rows, :])
    outer = jnp.transpose(outer)
    send_left[...] = outer[0:HALO, :]
    send_right[...] = outer[LANES - HALO :, :]

    upright = land[...]
    if count_words < LANES:
        filler = jnp.zeros((LANES - count_words, rows), jnp.int32)
        upright = jnp.concatenate([upright, filler], axis=0)
    words[HALO : HALO + rows, :] = jnp.transpose(upright)

    pl.semaphore_wait(barrier, len(near))

    first_words = land.at[0:1, :]
    last_words = land.at[count_words - 1 : count_words, :]
    own_lanes = pl.ds(LANES, rows)
    top_lanes = pl.ds(0, LANES)
    bottom_lanes = pl.ds(LANES + rows, LANES)
    ahead = pl.ds(0, LANES)
    behind = pl.ds(rows - LANES, LANES)
    right_side = side.at[0:HALO, :]
    left_side = side.at[LANES - HALO :, :]
    right_words = side_words.at[0:1, :]
    left_words = side_words.at[1:2, :]
    across_plan = (
        (send_left, right_side.at[:, own_lanes], (0, -1)),
        (send_right, left_side.at[:, own_lanes], (0, 1)),
        (first_words, right_words.at[:, own_lanes], (0, -1)),
        (last_words, left_words.at[:, own_lanes], (0, 1)),
    )
    down_across_plan = (
        (send_left.at[:, behind], right_side.at[:, top_lanes], (1, -1)),
        (send_right.at[:, behind], left_side.at[:, top_lanes], (1, 1)),
    )
    down_words_plan = (
        (first_words.at[:, behind], right_words.at[:, top_lanes], (1, -1)),
        (last_words.at[:, behind], left_words.at[:, top_lanes], (1, 1)),
    )
    up_across_plan = (
        (send_left.at[:, ahead], right_side.at[:, bottom_lanes], (-1, -1)),
        (send_right.at[:, ahead], left_side.at[:, bottom_lanes], (-1, 1)),
    )
    up_words_plan = (
        (first_words.at[:, ahead], right_words.at[:, bottom_lanes], (-1, -1)),
        (last_words.at[:, ahead], left_words.at[:, bottom_lanes], (-1, 1)),
    )
    down_plan = (
        (fine.at[:, rows : rows + HALO, :], fine.at[:, 0:HALO, :], (1, 0)),
        (words.at[rows : rows + HALO, :], words.at[0:HALO, :], (1, 0)),
    )
    up_plan = (
        (fine.at[:, HALO : 2 * HALO, :], fine.at[:, HALO + rows :, :], (-1, 0)),
        (words.at[HALO : 2 * HALO, :], words.at[HALO + rows :, :], (-1, 0)),
    )
    plans = (
        across_plan,
        down_across_plan,
        up_across_plan,
        down_words_plan,
        up_words_plan,
        down_plan,
        up_plan,
    )
    downs, ups = (1, 3, 5), (2, 4, 6)

    def settle_halo(which, sem):
        moved = sum(math.prod(source.shape) for source, _, _ in plans[which])
        if moved % (8 * LANES):
            settle(side_words.at[0:1, 0:moved], sem.at[which])
        else:
            settle(fine.at[0, 0 : moved // LANES, :], sem.at[which])

    def copies(which, taken):
        return [
            pltpu.make_async_remote_copy(
                src_ref=source,
                dst_ref=target,
                send_sem=halo_send.at[which],
                recv_sem=halo_recv.at[which],
                device_id=device(down, right),
                device_id_type=MESH,
            )
            for source, target, (down, right) in plans[which][taken]
        ]

    def send(which, taken=slice(None)):
        for copy in copies(which, taken):
            copy.start()

    send(0, slice(0, None, 2))
    send(0, slice(1, None, 2))

    @pl.when(has_below)
    def _():
        pl.semaphore_signal(
            from_above_sem, inc=1, device_id=device(1, 0), device_id_type=MESH
        )

    @pl.when(has_above)
    def _():
        pl.semaphore_signal(
            from_below_sem, inc=1, device_id=device(-1, 0), device_id_type=MESH
        )

    for right in range(1, col_devices):
        pl.semaphore_signal(
            column_sem, inc=1, device_id=device(0, right), device_id_type=MESH
        )

    settle(fine.at[1 : tiles - 1, HALO : HALO + rows, :], load_sem.at[2])
    @pl.when(has_below)
    def _():
        send(5)

    @pl.when(has_above)
    def _():
        send(6)

    @pl.when(has_below)
    def _():
        pl.semaphore_wait(from_below_sem, 1)

    @pl.when(has_above)
    def _():
        pl.semaphore_wait(from_above_sem, 1)

    for side_at in range(2):
        taken = slice(side_at, None, 2)

        @pl.when(has_below)
        def _():
            send(1, taken)
            send(3, taken)

        @pl.when(has_above)
        def _():
            send(2, taken)
            send(4, taken)

    blocks = rows // LANES + 2
    packed = cos_rows.shape
    row_index = (
        row_at * rows
        - LANES
        + lax.broadcasted_iota(jnp.int32, packed, 0) * LANES
        + lax.broadcasted_iota(jnp.int32, packed, 1)
    )
    latitude = ((row_index.astype(f32) + 0.5) / total_rows - 0.5) * math.pi
    on_globe = jnp.logical_and(row_index >= 0, row_index < total_rows)
    cos_rows[...] = jnp.where(on_globe, jnp.cos(latitude), 0.0)

    def placed(block):
        if block == 0:
            return slice(LANES - HALO, LANES), 0
        if block == blocks - 1:
            return slice(0, HALO), HALO + rows
        return slice(0, LANES), HALO + (block - 1) * LANES

    for block in range(blocks):
        taken, at = placed(block)
        spread = jnp.broadcast_to(cos_rows[block : block + 1, :], (LANES, LANES))
        cosines[at : at + taken.stop - taken.start, :] = jnp.transpose(spread)[taken, :]

    for product, cover, width in ((p0, c0, 8), (p1, c1, 16), (p2, c2, 16), (p3, c3, 16)):
        for ref in (product, cover):
            shape = (ref.shape[0], width, LANES)
            ref[:, 0:width, :] = jnp.zeros(shape, f32)
            ref[:, ref.shape[1] - width :, :] = jnp.zeros(shape, f32)

    def decode(tile, start, count):
        lanes = lax.broadcasted_iota(jnp.int32, (count, LANES), 1)
        place = tile * (LANES // 32) + lax.shift_right_logical(lanes, 5)
        word = jnp.take_along_axis(
            words[pl.ds(start, count), :], place, axis=1, mode="promise_in_bounds"
        )
        bit = lax.shift_left(jnp.ones_like(lanes), jnp.bitwise_and(lanes, 31))
        cover = jnp.where(
            jnp.bitwise_and(word, bit) != 0, cosines[pl.ds(start, count), :], 0.0
        )
        c0[tile, pl.ds(8 + start, count), :] = cover
        p0[tile, pl.ds(8 + start, count), :] = cover * fine[tile, pl.ds(start, count), :]

    sources = ((p0, c0), (p1, c1), (p2, c2), (p3, c3))
    partials = (partial0, partial1, partial2, partial3)
    outputs = (level_one, level_two, level_three, level_four)

    def filtered(level, tile, first, count):
        halves = []
        for ref in sources[level]:
            taps = [ref[tile, pl.ds(7 + a + 2 * first, count, stride=2), :] for a in range(4)]
            down = (taps[0] + taps[3]) + 3.0 * (taps[1] + taps[2])
            high = down.astype(bf16)
            halves += [high, (down - high.astype(f32)).astype(bf16)]
        return halves

    def table(tap, keep=True):
        weight = jnp.where(
            jnp.logical_or(tap == 0, tap == 3),
            stencil_weights[0] / 8.0,
            jnp.where(jnp.logical_or(tap == 1, tap == 2), stencil_weights[1] / 8.0, 0.0),
        )
        return jnp.where(keep, weight, 0.0).astype(bf16)

    band_row = lax.broadcasted_iota(jnp.int32, (4 * LANES, LANES), 0)
    band_col = lax.broadcasted_iota(jnp.int32, (4 * LANES, LANES), 1)
    band = table(band_row - (LANES - 1) - 2 * band_col)

    half = LANES // 2

    def column(at):
        middle = jnp.where(at == half, 0, -1)
        away = jnp.where(at > half, at - LANES, at)
        return jnp.where(jnp.logical_or(at == half, at == half - 1), middle, away)

    lane_in = lax.broadcasted_iota(jnp.int32, (LANES, LANES), 0)
    fine_in = jnp.where(
        lane_in < half, lane_in % HALO, LANES - 1 - (LANES - 1 - lane_in) % HALO
    )
    lane_out = lax.broadcasted_iota(jnp.int32, (LANES, LANES), 1)
    leftward = lane_out >= half
    from_side = table(
        column(lane_in) - 2 * column(lane_out) + 1, (lane_in >= half) == leftward
    )
    from_side_fine = table(
        column(fine_in) - 2 * column(lane_out) + 1, (lane_in >= half) == leftward
    )
    from_first = table(lane_in - 2 * column(lane_out) + 1, leftward)
    from_last = table(lane_in - LANES - 2 * column(lane_out) + 1, jnp.logical_not(leftward))

    def across(count, parts):
        result = None
        for operand, weights in parts:
            part = jnp.dot(operand, weights, preferred_element_type=f32)
            result = part if result is None else result + part
        num = result[0:count] + result[count : 2 * count]
        den = result[2 * count : 3 * count] + result[3 * count :]
        return num, den

    def own_parts(tile, tiles_in):
        start = max(2 * tile - 1, 0)
        stop = min(2 * tile + 3, tiles_in)
        skip = start - (2 * tile - 1)
        return start, stop, band[skip * LANES : (skip + stop - start) * LANES]

    def finish(num, den):
        value = num / jnp.maximum(den, floor_value)
        return value, den, den * value

    def ring(shape, tile, count_tiles):
        lanes = lax.broadcasted_iota(jnp.int32, shape, 1)
        if tile == count_tiles:
            return jnp.logical_or(lanes == half, lanes == half - 1)
        here = None
        if tile == 0:
            here = lanes == 0
        if tile == count_tiles - 1:
            final = lanes == LANES - 1
            here = final if here is None else jnp.logical_or(here, final)
        return here

    def tally(stat, value, cover, product):
        def parts(array):
            return array.reshape(array.shape[0] // 8, 8, LANES)

        weighted, total, largest = stat
        return (
            weighted + jnp.sum(parts(product), axis=0),
            total + jnp.sum(parts(cover), axis=0),
            jnp.maximum(largest, jnp.max(parts(value), axis=0)),
        )

    def masked(level, tile, value, cover, product):
        count_tiles = outputs[level].shape[1] // LANES
        here = ring(value.shape, tile, count_tiles)
        if tile == count_tiles:
            inside = jnp.where(here, value, -jnp.inf)
            return cover, product, (inside, jnp.where(here, cover, 0.0), jnp.where(here, product, 0.0))
        if here is not None:
            value = jnp.where(here, -jnp.inf, value)
            cover = jnp.where(here, 0.0, cover)
            product = jnp.where(here, 0.0, product)
        return cover, product, (value, cover, product)

    zero = jnp.zeros((8, LANES), f32)
    stats = [(zero, zero, jnp.full((8, LANES), -jnp.inf, f32)) for _ in range(LEVELS)]
    above_factor = jnp.where(has_above, 1.0, 0.0).astype(f32)
    below_factor = jnp.where(has_below, 1.0, 0.0).astype(f32)

    def inner_rows(level):
        return outputs[level].shape[0] + 16 - 2 * EDGE

    def inner_tile(level, tile, num, den, first=0):
        inner = num.shape[0]
        value, cover, product = finish(num, den)
        cover, product, counted = masked(level, tile, value, cover, product)
        if level + 1 < LEVELS:
            for ref, array in zip(sources[level + 1], (product, cover)):
                ref[tile, 16 + EDGE + first : 16 + EDGE + first + inner, :] = array
        stats[level] = tally(stats[level], *counted)
        return value

    for level in range(LEVELS):
        inner = inner_rows(level)
        tiles_in = sources[level][0].shape[0] - 1
        tiles_out = outputs[level].shape[1] // LANES

        def feed(tile):
            if level == 0:
                for start in range(0, rows, 64):
                    decode(tile, HALO + start, 64)
            operands.append(jnp.concatenate(filtered(level, tile, EDGE, inner), axis=0))

        operands = []
        fed = 0
        for tile in range(tiles_out):
            while fed < min(2 * tile + 3, tiles_in):
                feed(fed)
                fed += 1
            start, stop, weights = own_parts(tile, tiles_in)
            parts = ((jnp.concatenate(operands[start:stop], axis=1), weights),)
            value = inner_tile(level, tile, *across(inner, parts))
            lanes = slice(tile * LANES, (tile + 1) * LANES)
            outputs[level][EDGE - 8 : EDGE - 8 + inner, lanes] = value
        parts = (
            (operands[0], from_first),
            (operands[tiles_in - 1], from_last),
        )
        num, den = across(inner, parts)
        partials[level][0] = num
        partials[level][1] = den

    @pl.when(has_below)
    def _():
        settle_halo(6, halo_recv)

    @pl.when(has_above)
    def _():
        settle_halo(5, halo_recv)

    settle_halo(0, halo_recv)

    @pl.when(has_below)
    def _():
        settle_halo(2, halo_recv)
        settle_halo(4, halo_recv)

    @pl.when(has_above)
    def _():
        settle_halo(1, halo_recv)
        settle_halo(3, halo_recv)

    sub = lax.broadcasted_iota(jnp.int32, (HALO, LANES), 0)
    turned_lane = lax.broadcasted_iota(jnp.int32, (LANES, LANES), 1)
    turned_slot = jnp.minimum(turned_lane, LANES - 1 - turned_lane) // HALO
    filler = jnp.zeros((LANES - 8 * HALO, LANES), f32)
    for pair in range(blocks // 2):
        both = (pair, blocks - 1 - pair)
        ends = ([], [])
        for block in both:
            here = slice(block * LANES, (block + 1) * LANES)
            turn = jnp.broadcast_to(cos_rows[block : block + 1, :], (HALO, LANES))
            for index, (at, shift) in enumerate(((0, 0), (LANES - HALO, 32 - HALO))):
                word = jnp.broadcast_to(side_words[index : index + 1, here], (HALO, LANES))
                flag = jnp.bitwise_and(lax.shift_right_logical(word, sub + shift), 1)
                cover = jnp.where(flag != 0, turn, 0.0)
                ends[index].extend((cover, cover * side[at : at + HALO, here]))
        pieces = ends[0] + ([filler] if filler.shape[0] else []) + ends[1][::-1]
        flat = jnp.transpose(jnp.concatenate(pieces, axis=0))
        for index, block in enumerate(both):
            taken, at = placed(block)
            size = taken.stop - taken.start
            for kind, ref in ((0, c0), (1, p0)):
                held = jnp.where(turned_slot == 2 * index + kind, flat, 0.0)
                ref[tiles, 8 + at : 8 + at + size, :] = held[taken, :]

    for tile in range(tiles):
        decode(tile, 0, HALO)
        decode(tile, HALO + rows, HALO)

    def keep_strip(level, tile, cover, product):
        inner = inner_rows(level)
        own = outputs[level].shape[0]
        if level + 1 < LEVELS:
            for ref, array in zip(sources[level + 1], (product, cover)):
                ref[tile, 16:24, :] = array[0:8] * above_factor
                ref[tile, 24 : 16 + EDGE, :] = array[8:EDGE]
                ref[tile, 16 + EDGE + inner : 24 + own, :] = array[EDGE : 2 * EDGE - 8]
                ref[tile, 24 + own : 32 + own, :] = array[2 * EDGE - 8 :] * below_factor

    def strip(level, tile):
        top = filtered(level, tile, 0, EDGE)
        bottom = filtered(level, tile, EDGE + inner_rows(level), EDGE)
        return [piece for pair in zip(top, bottom) for piece in pair]

    middle = slice(8, 2 * EDGE - 8)
    def across_side(level, halves):
        weights = from_side_fine if level == 0 else from_side
        weights = jnp.concatenate([weights, weights], axis=0)
        high = jnp.concatenate(halves[0 : len(halves) // 4] + halves[len(halves) // 2 : -(len(halves) // 4)], axis=0)
        low = jnp.concatenate(halves[len(halves) // 4 : len(halves) // 2] + halves[-(len(halves) // 4) :], axis=0)
        count = high.shape[0] // 2
        result = jnp.dot(
            jnp.concatenate([high, low], axis=1), weights, preferred_element_type=f32
        )
        return result[0:count], result[count:]

    ring_values = []
    for level in range(LEVELS):
        output = outputs[level]
        own = output.shape[0]
        tiles_in = sources[level][0].shape[0] - 1
        tiles_out = output.shape[1] // LANES
        strips = [jnp.concatenate(strip(level, tile), axis=0) for tile in range(tiles_in)]
        for tile in range(tiles_out):
            start, stop, weights = own_parts(tile, tiles_in)
            parts = ((jnp.concatenate(strips[start:stop], axis=1), weights),)
            value, cover, product = finish(*across(2 * EDGE, parts))
            cover, product, counted = masked(level, tile, value, cover, product)
            keep_strip(level, tile, cover, product)
            stats[level] = tally(stats[level], *(array[middle] for array in counted))
            lanes = slice(tile * LANES, (tile + 1) * LANES)
            output[0 : EDGE - 8, lanes] = value[8:EDGE]
            output[own - EDGE + 8 :, lanes] = value[EDGE : 2 * EDGE - 8]
        parts = ((strips[tiles_in - 1], from_last), (strips[0], from_first))
        edge_partial = across(2 * EDGE, parts)
        inner = inner_rows(level)
        inner_values = []
        for first in range(0, inner, CHUNK):
            count = min(CHUNK, inner - first)
            num, den = across_side(level, filtered(level, tiles_in, EDGE + first, count))
            here = slice(first, first + count)
            num, den = num + partials[level][0, here, :], den + partials[level][1, here, :]
            inner_values.append(inner_tile(level, tiles_out, num, den, first))
        inner_value = jnp.concatenate(inner_values, axis=0)
        num, den = across_side(level, strip(level, tiles_in))
        num, den = num + edge_partial[0], den + edge_partial[1]
        value, cover, product = finish(num, den)
        cover, product, counted = masked(level, tiles_out, value, cover, product)
        keep_strip(level, tiles_out, cover, product)
        stats[level] = tally(stats[level], *(array[middle] for array in counted))
        ring_values.append((inner_value, value[middle]))

    lane = lax.broadcasted_iota(jnp.int32, (8, LANES), 1)
    row = lax.broadcasted_iota(jnp.int32, (8, LANES), 0)
    mine = zero
    for level, (weighted, total, largest) in enumerate(stats):
        weighted = jnp.sum(weighted, axis=0, keepdims=True)
        total = jnp.sum(total, axis=0, keepdims=True)
        sums = jnp.sum(jnp.where(row == 0, weighted, total), axis=1, keepdims=True)
        largest = jnp.max(largest, axis=0, keepdims=True)
        largest = jnp.max(jnp.broadcast_to(largest, (8, LANES)), axis=1, keepdims=True)
        mine = jnp.where(lane == level, jnp.where(row < 2, sums, largest), mine)
    stat_own[...] = mine
    pl.semaphore_wait(column_sem, col_devices - 1)
    far_first = sorted(enumerate(others), key=lambda other: (other[1][1] == 0, other[1][1]))
    for place, (down, right) in far_first:
        copy = pltpu.make_async_remote_copy(
            src_ref=stat_own.at[0:4],
            dst_ref=stat_all.at[place, 0:4],
            send_sem=stat_send,
            recv_sem=stat_recv,
            device_id=device(down, right),
            device_id_type=MESH,
        )
        copy.start()

    for output, (inner_value, edge_value) in zip(outputs, ring_values):
        own, width = output.shape
        tiles_out = width // LANES
        for start, array in (
            (0, edge_value[0:8]),
            (8, inner_value),
            (own - 8, edge_value[8:16]),
        ):
            turned = pltpu.roll(array, half, axis=1)
            here = slice(start, start + array.shape[0])
            for tile in sorted({0, tiles_out - 1}):
                lanes = slice(tile * LANES, (tile + 1) * LANES)
                at_ring = ring(array.shape, tile, tiles_out)
                output[here, lanes] = jnp.where(at_ring, turned, output[here, lanes])

    settle_halo(0, halo_send)

    @pl.when(has_below)
    def _():
        for which in downs:
            settle_halo(which, halo_send)

    @pl.when(has_above)
    def _():
        for which in ups:
            settle_halo(which, halo_send)

    arrived = stat_all.at[:, 0:4, :]
    settle(arrived, stat_recv)

    def combine(reduce):
        parts = [stat_own[0:4, :]] + [stat_all[place, 0:4, :] for place in range(len(others))]
        while len(parts) > 1:
            pairs = [reduce(*pair) for pair in zip(parts[0::2], parts[1::2])]
            parts = pairs + parts[2 * len(pairs) :]
        return parts[0]

    summed, largest = combine(jnp.add), combine(jnp.maximum)
    means_ref[...] = jnp.sum(summed[0:1] / (summed[1:2] + mean_eps), axis=0)[0:LEVELS]
    maxima_ref[...] = jnp.sum(largest[2:3], axis=0)[0:LEVELS]
    settle(arrived, stat_send)


def per_device(row_devices, col_devices, surface_field, land_words):
    rows, cols = surface_field.shape
    tiles = cols // LANES
    levels = tuple(
        jax.ShapeDtypeStruct((rows >> level, cols >> level), f32) for level in range(1, LEVELS + 1)
    )
    blocks = rows // LANES + 2
    scratch = [
        pltpu.VMEM((tiles, rows + 2 * HALO, LANES), f32),
        pltpu.VMEM((land_words.shape[1], rows), jnp.int32),
        pltpu.VMEM((rows + 2 * HALO, LANES), jnp.int32),
        pltpu.VMEM((rows + 2 * HALO, LANES), f32),
        pltpu.VMEM((8 * (-(-blocks // 8)), LANES), f32),
        pltpu.VMEM((HALO, rows), f32),
        pltpu.VMEM((HALO, rows), f32),
        pltpu.VMEM((LANES, rows + 2 * LANES), f32),
        pltpu.VMEM((8, rows + 2 * LANES), jnp.int32),
    ]
    for level in range(LEVELS):
        shape = ((cols >> level) // LANES + 1, (rows >> level) + 48, LANES)
        scratch += [pltpu.VMEM(shape, f32)] * 2
    for level in range(LEVELS):
        inner = (rows >> (level + 1)) + 16 - 2 * EDGE
        scratch.append(pltpu.VMEM((2, inner, LANES), f32))
    others = row_devices * col_devices - 1
    scratch += [
        pltpu.VMEM((8, LANES), f32),
        pltpu.VMEM((others, 8, LANES), f32),
        pltpu.SemaphoreType.DMA((3,)),
        pltpu.SemaphoreType.DMA,
        pltpu.SemaphoreType.DMA((7,)),
        pltpu.SemaphoreType.DMA((7,)),
        pltpu.SemaphoreType.DMA,
        pltpu.SemaphoreType.DMA,
        pltpu.SemaphoreType.REGULAR,
        pltpu.SemaphoreType.REGULAR,
        pltpu.SemaphoreType.REGULAR,
    ]
    vmem = pl.BlockSpec(memory_space=pltpu.VMEM)
    small = jax.ShapeDtypeStruct((LEVELS,), f32)
    results = (*levels, small, small)
    found = pl.pallas_call(
        functools.partial(kernel, row_devices, col_devices),
        out_shape=tuple(pltpu.VMEM(each.shape, each.dtype) for each in results),
        in_specs=[pl.BlockSpec(memory_space=pltpu.HBM)] * 2,
        out_specs=(vmem,) * len(results),
        scratch_shapes=scratch,
        compiler_params=pltpu.CompilerParams(
            collective_id=0, has_side_effects=True, vmem_limit_bytes=56 * 1024 * 1024
        ),
        name="coarsen_levels",
    )(surface_field, land_words.T)

    return pl.pallas_call(
        hand_over,
        out_shape=results,
        in_specs=[vmem] * len(results),
        out_specs=(pl.BlockSpec(memory_space=pl.ANY),) * len(results),
        scratch_shapes=[pltpu.SemaphoreType.DMA((len(results),))],
        compiler_params=pltpu.CompilerParams(vmem_limit_bytes=8 * 1024 * 1024),
        name="hand_over",
    )(*found)


def hand_over(*refs):
    count = LEVELS + 2
    sources, targets, sems = refs[:count], refs[count : 2 * count], refs[2 * count]
    copies = [
        pltpu.make_async_copy(sources[at], targets[at], sems.at[at]) for at in range(count)
    ]
    for copy in copies:
        copy.start()
    for copy in copies:
        copy.wait()


def solution(mesh):
    return jax.shard_map(
        functools.partial(per_device, mesh.shape["rows"], mesh.shape["cols"]),
        mesh=mesh,
        in_specs=(P("rows", "cols"), P("rows", "cols")),
        out_specs=(P("rows", "cols"),) * LEVELS + (P(), P()),
        check_vma=False,
    )
```

```python
import functools
import math

import jax
import jax.numpy as jnp
from jax import lax
from jax.experimental import pallas as pl
from jax.experimental.pallas import tpu as pltpu
from jax.sharding import PartitionSpec as P

stencil_weights = (0.125, 0.375, 0.375, 0.125)
floor_value = 0.05
mean_eps = 1e-06
LEVELS = 4
LANES = 128
HALO = 16
EDGE = 16
CHUNK = 80
MESH = pl.DeviceIdType.MESH
f32 = jnp.float32
bf16 = jnp.bfloat16


def kernel(
    row_devices,
    col_devices,
    field,
    land_words,
    level_one,
    level_two,
    level_three,
    level_four,
    means_ref,
    maxima_ref,
    fine,
    land,
    words,
    cosines,
    cos_rows,
    send_left,
    send_right,
    side,
    side_words,
    p0,
    c0,
    p1,
    c1,
    p2,
    c2,
    p3,
    c3,
    partial0,
    partial1,
    partial2,
    partial3,
    stat_own,
    stat_all,
    load_sem,
    land_sem,
    halo_send,
    halo_recv,
    stat_send,
    stat_recv,
    column_sem,
    from_above_sem,
    from_below_sem,
):
    rows, cols = field.shape
    tiles = cols // LANES
    count_words = land.shape[0]
    row_at = lax.axis_index("rows")
    col_at = lax.axis_index("cols")
    total_rows = rows * row_devices
    has_above = row_at > 0
    has_below = row_at < row_devices - 1

    def device(down, right):
        return (
            lax.rem(row_at + down + row_devices, row_devices),
            lax.rem(col_at + right + col_devices, col_devices),
        )

    others = [
        (down, right)
        for down in range(row_devices)
        for right in range(col_devices)
        if (down, right) != (0, 0)
    ]

    near = [(down, right) for down, right in others if down == 0 or right == 0]

    land_load = pltpu.make_async_copy(land_words, land, land_sem)

    def load(tile):
        start = tile * LANES
        return pltpu.make_async_copy(
            field.at[:, pl.ds(start, LANES)],
            fine.at[tile, pl.ds(HALO, rows), :],
            load_sem.at[0 if tile == 0 else 2 if tile < tiles - 1 else 1],
        )

    def settle(ref, sem):
        pltpu.make_async_copy(ref, ref, sem).wait()

    load(0).start()
    load(tiles - 1).start()
    land_load.start()

    barrier = pltpu.get_barrier_semaphore()
    for down, right in near:
        pl.semaphore_signal(barrier, inc=1, device_id=device(down, right), device_id_type=MESH)

    for tile in range(1, tiles - 1):
        load(tile).start()

    def clear(row_start, lane_start):
        fine[:, row_start : row_start + HALO, :] = jnp.zeros((tiles, HALO, LANES), f32)
        words[row_start : row_start + HALO, :] = jnp.zeros((HALO, LANES), jnp.int32)
        here = slice(lane_start, lane_start + LANES)
        side[0:HALO, here] = jnp.zeros((HALO, LANES), f32)
        side[LANES - HALO :, here] = jnp.zeros((HALO, LANES), f32)
        side_words[:, here] = jnp.zeros((8, LANES), jnp.int32)

    @pl.when(jnp.logical_not(has_above))
    def _():
        clear(0, 0)

    @pl.when(jnp.logical_not(has_below))
    def _():
        clear(HALO + rows, LANES + rows)

    load(0).wait()
    load(tiles - 1).wait()
    land_load.wait()
    own_rows = pl.ds(HALO, rows)
    lanes = lax.broadcasted_iota(jnp.int32, (rows, LANES), 1)
    outer = jnp.where(lanes < LANES // 2, fine[0, own_rows, :], fine[tiles - 1, own_rows, :])
    outer = jnp.transpose(outer)
    send_left[...] = outer[0:HALO, :]
    send_right[...] = outer[LANES - HALO :, :]

    upright = land[...]
    if count_words < LANES:
        filler = jnp.zeros((LANES - count_words, rows), jnp.int32)
        upright = jnp.concatenate([upright, filler], axis=0)
    words[HALO : HALO + rows, :] = jnp.transpose(upright)

    pl.semaphore_wait(barrier, len(near))

    first_words = land.at[0:1, :]
    last_words = land.at[count_words - 1 : count_words, :]
    own_lanes = pl.ds(LANES, rows)
    top_lanes = pl.ds(0, LANES)
    bottom_lanes = pl.ds(LANES + rows, LANES)
    ahead = pl.ds(0, LANES)
    behind = pl.ds(rows - LANES, LANES)
    right_side = side.at[0:HALO, :]
    left_side = side.at[LANES - HALO :, :]
    right_words = side_words.at[0:1, :]
    left_words = side_words.at[1:2, :]
    across_plan = (
        (send_left, right_side.at[:, own_lanes], (0, -1)),
        (send_right, left_side.at[:, own_lanes], (0, 1)),
        (first_words, right_words.at[:, own_lanes], (0, -1)),
        (last_words, left_words.at[:, own_lanes], (0, 1)),
    )
    down_across_plan = (
        (send_left.at[:, behind], right_side.at[:, top_lanes], (1, -1)),
        (send_right.at[:, behind], left_side.at[:, top_lanes], (1, 1)),
    )
    down_words_plan = (
        (first_words.at[:, behind], right_words.at[:, top_lanes], (1, -1)),
        (last_words.at[:, behind], left_words.at[:, top_lanes], (1, 1)),
    )
    up_across_plan = (
        (send_left.at[:, ahead], right_side.at[:, bottom_lanes], (-1, -1)),
        (send_right.at[:, ahead], left_side.at[:, bottom_lanes], (-1, 1)),
    )
    up_words_plan = (
        (first_words.at[:, ahead], right_words.at[:, bottom_lanes], (-1, -1)),
        (last_words.at[:, ahead], left_words.at[:, bottom_lanes], (-1, 1)),
    )
    down_plan = (
        (fine.at[:, rows : rows + HALO, :], fine.at[:, 0:HALO, :], (1, 0)),
        (words.at[rows : rows + HALO, :], words.at[0:HALO, :], (1, 0)),
    )
    up_plan = (
        (fine.at[:, HALO : 2 * HALO, :], fine.at[:, HALO + rows :, :], (-1, 0)),
        (words.at[HALO : 2 * HALO, :], words.at[HALO + rows :, :], (-1, 0)),
    )
    plans = (
        across_plan,
        down_across_plan,
        up_across_plan,
        down_words_plan,
        up_words_plan,
        down_plan,
        up_plan,
    )
    downs, ups = (1, 3, 5), (2, 4, 6)

    def settle_halo(which, sem):
        moved = sum(math.prod(source.shape) for source, _, _ in plans[which])
        if moved % (8 * LANES):
            settle(side_words.at[0:1, 0:moved], sem.at[which])
        else:
            settle(fine.at[0, 0 : moved // LANES, :], sem.at[which])

    def copies(which, taken):
        return [
            pltpu.make_async_remote_copy(
                src_ref=source,
                dst_ref=target,
                send_sem=halo_send.at[which],
                recv_sem=halo_recv.at[which],
                device_id=device(down, right),
                device_id_type=MESH,
            )
            for source, target, (down, right) in plans[which][taken]
        ]

    def send(which, taken=slice(None)):
        for copy in copies(which, taken):
            copy.start()

    send(0, slice(0, None, 2))
    send(0, slice(1, None, 2))

    @pl.when(has_below)
    def _():
        pl.semaphore_signal(
            from_above_sem, inc=1, device_id=device(1, 0), device_id_type=MESH
        )

    @pl.when(has_above)
    def _():
        pl.semaphore_signal(
            from_below_sem, inc=1, device_id=device(-1, 0), device_id_type=MESH
        )

    for right in range(1, col_devices):
        pl.semaphore_signal(
            column_sem, inc=1, device_id=device(0, right), device_id_type=MESH
        )

    settle(fine.at[1 : tiles - 1, HALO : HALO + rows, :], load_sem.at[2])
    @pl.when(has_below)
    def _():
        send(5)

    @pl.when(has_above)
    def _():
        send(6)

    @pl.when(has_below)
    def _():
        pl.semaphore_wait(from_below_sem, 1)

    @pl.when(has_above)
    def _():
        pl.semaphore_wait(from_above_sem, 1)

    for side_at in range(2):
        taken = slice(side_at, None, 2)

        @pl.when(has_below)
        def _():
            send(1, taken)
            send(3, taken)

        @pl.when(has_above)
        def _():
            send(2, taken)
            send(4, taken)

    blocks = rows // LANES + 2
    packed = cos_rows.shape
    row_index = (
        row_at * rows
        - LANES
        + lax.broadcasted_iota(jnp.int32, packed, 0) * LANES
        + lax.broadcasted_iota(jnp.int32, packed, 1)
    )
    latitude = ((row_index.astype(f32) + 0.5) / total_rows - 0.5) * math.pi
    on_globe = jnp.logical_and(row_index >= 0, row_index < total_rows)
    cos_rows[...] = jnp.where(on_globe, jnp.cos(latitude), 0.0)

    def placed(block):
        if block == 0:
            return slice(LANES - HALO, LANES), 0
        if block == blocks - 1:
            return slice(0, HALO), HALO + rows
        return slice(0, LANES), HALO + (block - 1) * LANES

    for block in range(blocks):
        taken, at = placed(block)
        spread = jnp.broadcast_to(cos_rows[block : block + 1, :], (LANES, LANES))
        cosines[at : at + taken.stop - taken.start, :] = jnp.transpose(spread)[taken, :]

    for product, cover, width in ((p0, c0, 8), (p1, c1, 16), (p2, c2, 16), (p3, c3, 16)):
        for ref in (product, cover):
            shape = (ref.shape[0], width, LANES)
            ref[:, 0:width, :] = jnp.zeros(shape, f32)
            ref[:, ref.shape[1] - width :, :] = jnp.zeros(shape, f32)

    def decode(tile, start, count):
        lanes = lax.broadcasted_iota(jnp.int32, (count, LANES), 1)
        place = tile * (LANES // 32) + lax.shift_right_logical(lanes, 5)
        word = jnp.take_along_axis(
            words[pl.ds(start, count), :], place, axis=1, mode="promise_in_bounds"
        )
        bit = lax.shift_left(jnp.ones_like(lanes), jnp.bitwise_and(lanes, 31))
        cover = jnp.where(
            jnp.bitwise_and(word, bit) != 0, cosines[pl.ds(start, count), :], 0.0
        )
        c0[tile, pl.ds(8 + start, count), :] = cover
        p0[tile, pl.ds(8 + start, count), :] = cover * fine[tile, pl.ds(start, count), :]

    sources = ((p0, c0), (p1, c1), (p2, c2), (p3, c3))
    partials = (partial0, partial1, partial2, partial3)
    outputs = (level_one, level_two, level_three, level_four)

    def filtered(level, tile, first, count):
        halves = []
        for ref in sources[level]:
            taps = [ref[tile, pl.ds(7 + a + 2 * first, count, stride=2), :] for a in range(4)]
            down = (taps[0] + taps[3]) + 3.0 * (taps[1] + taps[2])
            high = down.astype(bf16)
            halves += [high, (down - high.astype(f32)).astype(bf16)]
        return halves

    def table(tap, keep=True):
        weight = jnp.where(
            jnp.logical_or(tap == 0, tap == 3),
            stencil_weights[0] / 8.0,
            jnp.where(jnp.logical_or(tap == 1, tap == 2), stencil_weights[1] / 8.0, 0.0),
        )
        return jnp.where(keep, weight, 0.0).astype(bf16)

    band_row = lax.broadcasted_iota(jnp.int32, (4 * LANES, LANES), 0)
    band_col = lax.broadcasted_iota(jnp.int32, (4 * LANES, LANES), 1)
    band = table(band_row - (LANES - 1) - 2 * band_col)

    half = LANES // 2

    def column(at):
        middle = jnp.where(at == half, 0, -1)
        away = jnp.where(at > half, at - LANES, at)
        return jnp.where(jnp.logical_or(at == half, at == half - 1), middle, away)

    lane_in = lax.broadcasted_iota(jnp.int32, (LANES, LANES), 0)
    fine_in = jnp.where(
        lane_in < half, lane_in % HALO, LANES - 1 - (LANES - 1 - lane_in) % HALO
    )
    lane_out = lax.broadcasted_iota(jnp.int32, (LANES, LANES), 1)
    leftward = lane_out >= half
    from_side = table(
        column(lane_in) - 2 * column(lane_out) + 1, (lane_in >= half) == leftward
    )
    from_side_fine = table(
        column(fine_in) - 2 * column(lane_out) + 1, (lane_in >= half) == leftward
    )
    from_first = table(lane_in - 2 * column(lane_out) + 1, leftward)
    from_last = table(lane_in - LANES - 2 * column(lane_out) + 1, jnp.logical_not(leftward))

    def across(count, parts):
        result = None
        for operand, weights in parts:
            part = jnp.dot(operand, weights, preferred_element_type=f32)
            result = part if result is None else result + part
        num = result[0:count] + result[count : 2 * count]
        den = result[2 * count : 3 * count] + result[3 * count :]
        return num, den

    def own_parts(tile, tiles_in):
        start = max(2 * tile - 1, 0)
        stop = min(2 * tile + 3, tiles_in)
        skip = start - (2 * tile - 1)
        return start, stop, band[skip * LANES : (skip + stop - start) * LANES]

    def finish(num, den):
        value = num / jnp.maximum(den, floor_value)
        return value, den, den * value

    def ring(shape, tile, count_tiles):
        lanes = lax.broadcasted_iota(jnp.int32, shape, 1)
        if tile == count_tiles:
            return jnp.logical_or(lanes == half, lanes == half - 1)
        here = None
        if tile == 0:
            here = lanes == 0
        if tile == count_tiles - 1:
            final = lanes == LANES - 1
            here = final if here is None else jnp.logical_or(here, final)
        return here

    def tally(stat, value, cover, product):
        def parts(array):
            return array.reshape(array.shape[0] // 8, 8, LANES)

        weighted, total, largest = stat
        return (
            weighted + jnp.sum(parts(product), axis=0),
            total + jnp.sum(parts(cover), axis=0),
            jnp.maximum(largest, jnp.max(parts(value), axis=0)),
        )

    def masked(level, tile, value, cover, product):
        count_tiles = outputs[level].shape[1] // LANES
        here = ring(value.shape, tile, count_tiles)
        if tile == count_tiles:
            inside = jnp.where(here, value, -jnp.inf)
            return cover, product, (inside, jnp.where(here, cover, 0.0), jnp.where(here, product, 0.0))
        if here is not None:
            value = jnp.where(here, -jnp.inf, value)
            cover = jnp.where(here, 0.0, cover)
            product = jnp.where(here, 0.0, product)
        return cover, product, (value, cover, product)

    zero = jnp.zeros((8, LANES), f32)
    stats = [(zero, zero, jnp.full((8, LANES), -jnp.inf, f32)) for _ in range(LEVELS)]
    above_factor = jnp.where(has_above, 1.0, 0.0).astype(f32)
    below_factor = jnp.where(has_below, 1.0, 0.0).astype(f32)

    def inner_rows(level):
        return outputs[level].shape[0] + 16 - 2 * EDGE

    def inner_tile(level, tile, num, den, first=0):
        inner = num.shape[0]
        value, cover, product = finish(num, den)
        cover, product, counted = masked(level, tile, value, cover, product)
        if level + 1 < LEVELS:
            for ref, array in zip(sources[level + 1], (product, cover)):
                ref[tile, 16 + EDGE + first : 16 + EDGE + first + inner, :] = array
        stats[level] = tally(stats[level], *counted)
        return value

    for level in range(LEVELS):
        inner = inner_rows(level)
        tiles_in = sources[level][0].shape[0] - 1
        tiles_out = outputs[level].shape[1] // LANES

        def feed(tile):
            if level == 0:
                for start in range(0, rows, 64):
                    decode(tile, HALO + start, 64)
            operands.append(jnp.concatenate(filtered(level, tile, EDGE, inner), axis=0))

        operands = []
        fed = 0
        for tile in range(tiles_out):
            while fed < min(2 * tile + 3, tiles_in):
                feed(fed)
                fed += 1
            start, stop, weights = own_parts(tile, tiles_in)
            parts = ((jnp.concatenate(operands[start:stop], axis=1), weights),)
            value = inner_tile(level, tile, *across(inner, parts))
            lanes = slice(tile * LANES, (tile + 1) * LANES)
            outputs[level][EDGE - 8 : EDGE - 8 + inner, lanes] = value
        parts = (
            (operands[0], from_first),
            (operands[tiles_in - 1], from_last),
        )
        num, den = across(inner, parts)
        partials[level][0] = num
        partials[level][1] = den

    @pl.when(has_below)
    def _():
        settle_halo(6, halo_recv)

    @pl.when(has_above)
    def _():
        settle_halo(5, halo_recv)

    settle_halo(0, halo_recv)

    @pl.when(has_below)
    def _():
        settle_halo(2, halo_recv)
        settle_halo(4, halo_recv)

    @pl.when(has_above)
    def _():
        settle_halo(1, halo_recv)
        settle_halo(3, halo_recv)

    sub = lax.broadcasted_iota(jnp.int32, (HALO, LANES), 0)
    turned_lane = lax.broadcasted_iota(jnp.int32, (LANES, LANES), 1)
    turned_slot = jnp.minimum(turned_lane, LANES - 1 - turned_lane) // HALO
    filler = jnp.zeros((LANES - 8 * HALO, LANES), f32)
    for pair in range(blocks // 2):
        both = (pair, blocks - 1 - pair)
        ends = ([], [])
        for block in both:
            here = slice(block * LANES, (block + 1) * LANES)
            turn = jnp.broadcast_to(cos_rows[block : block + 1, :], (HALO, LANES))
            for index, (at, shift) in enumerate(((0, 0), (LANES - HALO, 32 - HALO))):
                word = jnp.broadcast_to(side_words[index : index + 1, here], (HALO, LANES))
                flag = jnp.bitwise_and(lax.shift_right_logical(word, sub + shift), 1)
                cover = jnp.where(flag != 0, turn, 0.0)
                ends[index].extend((cover, cover * side[at : at + HALO, here]))
        pieces = ends[0] + ([filler] if filler.shape[0] else []) + ends[1][::-1]
        flat = jnp.transpose(jnp.concatenate(pieces, axis=0))
        for index, block in enumerate(both):
            taken, at = placed(block)
            size = taken.stop - taken.start
            for kind, ref in ((0, c0), (1, p0)):
                held = jnp.where(turned_slot == 2 * index + kind, flat, 0.0)
                ref[tiles, 8 + at : 8 + at + size, :] = held[taken, :]

    for tile in range(tiles):
        decode(tile, 0, HALO)
        decode(tile, HALO + rows, HALO)

    def keep_strip(level, tile, cover, product):
        inner = inner_rows(level)
        own = outputs[level].shape[0]
        if level + 1 < LEVELS:
            for ref, array in zip(sources[level + 1], (product, cover)):
                ref[tile, 16:24, :] = array[0:8] * above_factor
                ref[tile, 24 : 16 + EDGE, :] = array[8:EDGE]
                ref[tile, 16 + EDGE + inner : 24 + own, :] = array[EDGE : 2 * EDGE - 8]
                ref[tile, 24 + own : 32 + own, :] = array[2 * EDGE - 8 :] * below_factor

    def strip(level, tile):
        top = filtered(level, tile, 0, EDGE)
        bottom = filtered(level, tile, EDGE + inner_rows(level), EDGE)
        return [piece for pair in zip(top, bottom) for piece in pair]

    middle = slice(8, 2 * EDGE - 8)
    def across_side(level, halves):
        weights = from_side_fine if level == 0 else from_side
        weights = jnp.concatenate([weights, weights], axis=0)
        high = jnp.concatenate(halves[0 : len(halves) // 4] + halves[len(halves) // 2 : -(len(halves) // 4)], axis=0)
        low = jnp.concatenate(halves[len(halves) // 4 : len(halves) // 2] + halves[-(len(halves) // 4) :], axis=0)
        count = high.shape[0] // 2
        result = jnp.dot(
            jnp.concatenate([high, low], axis=1), weights, preferred_element_type=f32
        )
        return result[0:count], result[count:]

    ring_values = []
    for level in range(LEVELS):
        output = outputs[level]
        own = output.shape[0]
        tiles_in = sources[level][0].shape[0] - 1
        tiles_out = output.shape[1] // LANES
        strips = [jnp.concatenate(strip(level, tile), axis=0) for tile in range(tiles_in)]
        for tile in range(tiles_out):
            start, stop, weights = own_parts(tile, tiles_in)
            parts = ((jnp.concatenate(strips[start:stop], axis=1), weights),)
            value, cover, product = finish(*across(2 * EDGE, parts))
            cover, product, counted = masked(level, tile, value, cover, product)
            keep_strip(level, tile, cover, product)
            stats[level] = tally(stats[level], *(array[middle] for array in counted))
            lanes = slice(tile * LANES, (tile + 1) * LANES)
            output[0 : EDGE - 8, lanes] = value[8:EDGE]
            output[own - EDGE + 8 :, lanes] = value[EDGE : 2 * EDGE - 8]
        parts = ((strips[tiles_in - 1], from_last), (strips[0], from_first))
        edge_partial = across(2 * EDGE, parts)
        inner = inner_rows(level)
        inner_values = []
        for first in range(0, inner, CHUNK):
            count = min(CHUNK, inner - first)
            num, den = across_side(level, filtered(level, tiles_in, EDGE + first, count))
            here = slice(first, first + count)
            num, den = num + partials[level][0, here, :], den + partials[level][1, here, :]
            inner_values.append(inner_tile(level, tiles_out, num, den, first))
        inner_value = jnp.concatenate(inner_values, axis=0)
        num, den = across_side(level, strip(level, tiles_in))
        num, den = num + edge_partial[0], den + edge_partial[1]
        value, cover, product = finish(num, den)
        cover, product, counted = masked(level, tiles_out, value, cover, product)
        keep_strip(level, tiles_out, cover, product)
        stats[level] = tally(stats[level], *(array[middle] for array in counted))
        ring_values.append((inner_value, value[middle]))

    lane = lax.broadcasted_iota(jnp.int32, (8, LANES), 1)
    row = lax.broadcasted_iota(jnp.int32, (8, LANES), 0)
    mine = zero
    for level, (weighted, total, largest) in enumerate(stats):
        weighted = jnp.sum(weighted, axis=0, keepdims=True)
        total = jnp.sum(total, axis=0, keepdims=True)
        sums = jnp.sum(jnp.where(row == 0, weighted, total), axis=1, keepdims=True)
        largest = jnp.max(largest, axis=0, keepdims=True)
        largest = jnp.max(jnp.broadcast_to(largest, (8, LANES)), axis=1, keepdims=True)
        mine = jnp.where(lane == level, jnp.where(row < 2, sums, largest), mine)
    stat_own[...] = mine
    pl.semaphore_wait(column_sem, col_devices - 1)
    def send_stats(sign):
        order = sorted(enumerate(others), key=lambda other: (other[1][1] == 0, sign * other[1][1]))
        for place, (down, right) in order:
            pltpu.make_async_remote_copy(
                src_ref=stat_own.at[0:4],
                dst_ref=stat_all.at[place, 0:4],
                send_sem=stat_send,
                recv_sem=stat_recv,
                device_id=device(down, right),
                device_id_type=MESH,
            ).start()

    @pl.when(2 * col_at < col_devices)
    def _():
        send_stats(-1)

    @pl.when(2 * col_at >= col_devices)
    def _():
        send_stats(1)

    for output, (inner_value, edge_value) in zip(outputs, ring_values):
        own, width = output.shape
        tiles_out = width // LANES
        for start, array in (
            (0, edge_value[0:8]),
            (8, inner_value),
            (own - 8, edge_value[8:16]),
        ):
            turned = pltpu.roll(array, half, axis=1)
            here = slice(start, start + array.shape[0])
            for tile in sorted({0, tiles_out - 1}):
                lanes = slice(tile * LANES, (tile + 1) * LANES)
                at_ring = ring(array.shape, tile, tiles_out)
                output[here, lanes] = jnp.where(at_ring, turned, output[here, lanes])

    settle_halo(0, halo_send)

    @pl.when(has_below)
    def _():
        for which in downs:
            settle_halo(which, halo_send)

    @pl.when(has_above)
    def _():
        for which in ups:
            settle_halo(which, halo_send)

    arrived = stat_all.at[:, 0:4, :]
    settle(arrived, stat_recv)

    def combine(reduce):
        parts = [stat_own[0:4, :]] + [stat_all[place, 0:4, :] for place in range(len(others))]
        while len(parts) > 1:
            pairs = [reduce(*pair) for pair in zip(parts[0::2], parts[1::2])]
            parts = pairs + parts[2 * len(pairs) :]
        return parts[0]

    summed, largest = combine(jnp.add), combine(jnp.maximum)
    means_ref[...] = jnp.sum(summed[0:1] / (summed[1:2] + mean_eps), axis=0)[0:LEVELS]
    maxima_ref[...] = jnp.sum(largest[2:3], axis=0)[0:LEVELS]
    settle(arrived, stat_send)


def per_device(row_devices, col_devices, surface_field, land_words):
    rows, cols = surface_field.shape
    tiles = cols // LANES
    levels = tuple(
        jax.ShapeDtypeStruct((rows >> level, cols >> level), f32) for level in range(1, LEVELS + 1)
    )
    blocks = rows // LANES + 2
    scratch = [
        pltpu.VMEM((tiles, rows + 2 * HALO, LANES), f32),
        pltpu.VMEM((land_words.shape[1], rows), jnp.int32),
        pltpu.VMEM((rows + 2 * HALO, LANES), jnp.int32),
        pltpu.VMEM((rows + 2 * HALO, LANES), f32),
        pltpu.VMEM((8 * (-(-blocks // 8)), LANES), f32),
        pltpu.VMEM((HALO, rows), f32),
        pltpu.VMEM((HALO, rows), f32),
        pltpu.VMEM((LANES, rows + 2 * LANES), f32),
        pltpu.VMEM((8, rows + 2 * LANES), jnp.int32),
    ]
    for level in range(LEVELS):
        shape = ((cols >> level) // LANES + 1, (rows >> level) + 48, LANES)
        scratch += [pltpu.VMEM(shape, f32)] * 2
    for level in range(LEVELS):
        inner = (rows >> (level + 1)) + 16 - 2 * EDGE
        scratch.append(pltpu.VMEM((2, inner, LANES), f32))
    others = row_devices * col_devices - 1
    scratch += [
        pltpu.VMEM((8, LANES), f32),
        pltpu.VMEM((others, 8, LANES), f32),
        pltpu.SemaphoreType.DMA((3,)),
        pltpu.SemaphoreType.DMA,
        pltpu.SemaphoreType.DMA((7,)),
        pltpu.SemaphoreType.DMA((7,)),
        pltpu.SemaphoreType.DMA,
        pltpu.SemaphoreType.DMA,
        pltpu.SemaphoreType.REGULAR,
        pltpu.SemaphoreType.REGULAR,
        pltpu.SemaphoreType.REGULAR,
    ]
    vmem = pl.BlockSpec(memory_space=pltpu.VMEM)
    small = jax.ShapeDtypeStruct((LEVELS,), f32)
    results = (*levels, small, small)
    found = pl.pallas_call(
        functools.partial(kernel, row_devices, col_devices),
        out_shape=tuple(pltpu.VMEM(each.shape, each.dtype) for each in results),
        in_specs=[pl.BlockSpec(memory_space=pltpu.HBM)] * 2,
        out_specs=(vmem,) * len(results),
        scratch_shapes=scratch,
        compiler_params=pltpu.CompilerParams(
            collective_id=0, has_side_effects=True, vmem_limit_bytes=56 * 1024 * 1024
        ),
        name="coarsen_levels",
    )(surface_field, land_words.T)

    return pl.pallas_call(
        hand_over,
        out_shape=results,
        in_specs=[vmem] * len(results),
        out_specs=(pl.BlockSpec(memory_space=pl.ANY),) * len(results),
        scratch_shapes=[pltpu.SemaphoreType.DMA((len(results),))],
        compiler_params=pltpu.CompilerParams(vmem_limit_bytes=8 * 1024 * 1024),
        name="hand_over",
    )(*found)


def hand_over(*refs):
    count = LEVELS + 2
    sources, targets, sems = refs[:count], refs[count : 2 * count], refs[2 * count]
    copies = [
        pltpu.make_async_copy(sources[at], targets[at], sems.at[at]) for at in range(count)
    ]
    for copy in copies:
        copy.start()
    for copy in copies:
        copy.wait()


def solution(mesh):
    return jax.shard_map(
        functools.partial(per_device, mesh.shape["rows"], mesh.shape["cols"]),
        mesh=mesh,
        in_specs=(P("rows", "cols"), P("rows", "cols")),
        out_specs=(P("rows", "cols"),) * LEVELS + (P(), P()),
        check_vma=False,
    )
```
